64 devices in a mesh: batch: 4 (over x, y), col: 16 (over z, core).
Axes of the slice: x: 2, y: 2, z: 8, core: 2. Of those that a mesh axis runs over, the one named last changes fastest.
The devices are a block of a 4x4x8 slice.
Arguments:
- lower: bfloat16 [16384, 4096], P('batch', 'col'), parts along dimension 0
- rhs: bfloat16 [16384, 16384], P('batch', 'col'), parts along dimension 0
Outputs:
- output: bfloat16 [16384, 16384], P('batch', 'col'), parts along dimension 0
There are 4 independent parts. The reference program is written for one: setup_inputs(seed, part) draws one part's arguments, and reference() takes and returns one part's arrays. A program takes and returns all parts, laid end to end along the dimension named above; each array names one.
All inputs are finite; a program needn't handle non-finite values.
Results may differ from the reference program's by a relative error of at most 0.001.
Values are sent between devices in bfloat16 or wider.
A program may use at most 768 MiB of HBM per device.

```python
import jax
import jax.numpy as jnp
from jax import lax

N = 4096
BLOCK_SIZE = 256
GROUP = 16
COLS_DEV = 1024

PER_DEV = N // (BLOCK_SIZE * GROUP)
COLUMNS = COLS_DEV * GROUP


def setup_inputs(seed: int = 0, part: int = 0) -> dict:
    base_key = jax.random.fold_in(jax.random.key(seed), part)
    key_lower, key_rhs = jax.random.split(base_key)
    entries = jax.random.normal(key_lower, (N, N), jnp.float32)
    natural = jnp.tril(entries) * (N ** -0.5)
    stored = natural.reshape(N, PER_DEV, GROUP, BLOCK_SIZE).transpose(0, 2, 1, 3).reshape(N, N)
    rhs = jax.random.normal(key_rhs, (N, COLUMNS), jnp.float32)
    return {"lower": stored.astype(jnp.bfloat16), "rhs": rhs.astype(jnp.bfloat16)}


def reference(lower, rhs):
    natural = lower.reshape(N, GROUP, PER_DEV, BLOCK_SIZE).transpose(0, 2, 1, 3).reshape(N, N)
    col_groups = rhs.reshape(N, GROUP, COLS_DEV).transpose(1, 0, 2)

    def one_group(rhs_cols):
        return jnp.dot(natural, rhs_cols, preferred_element_type=jnp.float32).astype(jnp.bfloat16)

    results = lax.map(one_group, col_groups)
    return results.transpose(1, 0, 2).reshape(N, COLUMNS)
```

```python
import functools

import jax
import jax.numpy as jnp
from jax import lax
from jax.experimental import pallas as pl
from jax.experimental.pallas import tpu as pltpu
from jax.sharding import PartitionSpec as P

BLOCK = 256
MESH = pl.DeviceIdType.MESH
CHIPS = 8
PLUS_HOPS = (2, 2, 3, 5, 4, 4, 3, 2)
LONGER = {(0, 3): 12, (1, 3): 7, (1, 4): 13, (2, 4): 6, (2, 5): 9}
MORE_ODD = (2, 5)


def pick(index, values):
    out = jnp.int32(values[-1])
    for j in range(len(values) - 2, -1, -1):
        out = jnp.where(index == j, jnp.int32(values[j]), out)
    return out


def kernel(nb, l_ref, b_ref, acc, lv, bv, rsem, psem, msem, dsem, bsem):
    c = lax.axis_index("col")
    z, p = c // 2, c % 2
    q = 1 - p
    nxt = ((z + 1) % CHIPS) * 2 + p
    prv = ((z + CHIPS - 1) % CHIPS) * 2 + p
    mate = z * 2 + q

    def split(s, d, par):
        t = jnp.where(d <= pick(s, PLUS_HOPS), 0, nb)
        for (s0, d0), v in LONGER.items():
            v = v - par if (s0, d0) == MORE_ODD else v
            t = jnp.where(s * CHIPS + d == s0 * CHIPS + d0, v, t)
        return t

    def slot(k, i):
        return nb * k - k * (k - 1) // 2 + i - k

    def remote(src, t, sem, dev):
        return pltpu.make_async_remote_copy(
            src_ref=src, dst_ref=lv.at[t], send_sem=sem, recv_sem=rsem.at[t],
            device_id={"col": dev}, device_id_type=MESH)

    def own_rows(i):
        return l_ref.at[pl.ds(pl.multiple_of(i * BLOCK, BLOCK), BLOCK), :]

    def b_copy(k):
        rows = pl.ds(pl.multiple_of(k * BLOCK, BLOCK), BLOCK)
        return pltpu.make_async_copy(b_ref.at[rows, :], bv.at[rows, :], bsem.at[k])

    def land(t):
        remote(lv.at[t], t, psem.at[t], nxt).wait_recv()

    def plus_start(d, par):
        s = (z + CHIPS - d) % CHIPS
        return jnp.maximum(2 * s + par, split(s, d, par))

    def plus_next(d, i, par):
        more = i < nb - 1
        d2 = d + 1
        i2 = jnp.where(more, i + 1, plus_start(d2, par))
        ended = i >= nb
        return jnp.where(more | ended, d, d2), jnp.where(ended, i, i2)

    def minus_start(d, par):
        s = (z + d) % CHIPS
        k = 2 * s + par
        return jnp.where(split(s, CHIPS - d, par) > k, k, nb)

    def minus_next(d, i, par):
        s = (z + d) % CHIPS
        more = i + 1 < split(s, CHIPS - d, par)
        d2 = d + 1
        i2 = jnp.where(more, i + 1, minus_start(d2, par))
        ended = i >= nb
        return jnp.where(more | ended, d, d2), jnp.where(ended, i, i2)

    barrier = pltpu.get_barrier_semaphore()
    for dev in (nxt, prv, mate):
        pl.semaphore_signal(barrier, inc=1, device_id={"col": dev}, device_id_type=MESH)
    pl.semaphore_wait(barrier, 3)

    def send_own(i, carry):
        t = slot(c, i)
        remote(own_rows(i), t, psem.at[t], nxt).start()
        remote(own_rows(i), t, msem.at[t], prv).start()
        remote(own_rows(i), t, dsem.at[t], mate).start()
        pltpu.make_async_copy(own_rows(i), lv.at[t], rsem.at[t]).start()
        return carry

    lax.fori_loop(c, nb, send_own, 0)

    def load_b(k, carry):
        b_copy(k).start()
        return carry

    lax.fori_loop(0, nb, load_b, 0)

    def clear(i, carry):
        acc[pl.ds(pl.multiple_of(i * 64, 64), 64), :] = jnp.zeros((64, acc.shape[1]), jnp.float32)
        return carry

    lax.fori_loop(0, acc.shape[0] // 64, clear, 0)

    def wait_b(k, carry):
        b_copy(k).wait()
        return carry

    lax.fori_loop(0, nb, wait_b, 0)

    def multiply(k, i):
        t = slot(k, i)
        rows = pl.ds(pl.multiple_of(i * BLOCK, BLOCK), BLOCK)
        depth = pl.ds(pl.multiple_of(k * BLOCK, BLOCK), BLOCK)
        tile = lv[t]
        half = acc.shape[1] // 2
        for n in range(2):
            cols = slice(n * half, (n + 1) * half)
            acc[rows, cols] += jnp.dot(tile, bv[depth, cols], preferred_element_type=jnp.float32)

    slots = 36

    def step(n, cur):
        pd, pi, md, mi, qpd, qpi, qmd, qmi = cur
        ps, ms = (z + CHIPS - pd) % CHIPS, (z + md) % CHIPS
        pk, mk = 2 * ps + p, 2 * ms + p

        @pl.when(pi < nb)
        def _():
            t = slot(pk, pi)
            land(t)

            @pl.when(split(ps, pd + 1, p) <= pi)
            def _():
                remote(lv.at[t], t, psem.at[t], nxt).start()

            remote(lv.at[t], t, dsem.at[t], mate).start()

        @pl.when(mi < nb)
        def _():
            t = slot(mk, mi)
            land(t)

            @pl.when(split(ms, CHIPS - 1 - md, p) > mi)
            def _():
                remote(lv.at[t], t, msem.at[t], prv).start()

            remote(lv.at[t], t, dsem.at[t], mate).start()

        qps, qms = (z + CHIPS - qpd) % CHIPS, (z + qmd) % CHIPS
        late = n >= 1
        own = c + n
        other = mate + n
        ks = (pk, mk, 2 * qps + q, 2 * qms + q, c, mate)
        is_ = (pi, mi, jnp.where(late, qpi, nb), jnp.where(late, qmi, nb), own, other)

        def one(j, carry):
            k, i = ks[-1], is_[-1]
            for x in range(4, -1, -1):
                k = jnp.where(j == x, ks[x], k)
                i = jnp.where(j == x, is_[x], i)

            @pl.when(i < nb)
            def _():
                @pl.when(j >= 2)
                def _():
                    land(slot(k, i))

                multiply(k, i)

            return carry

        lax.fori_loop(0, 6, one, 0)

        npd, npi = plus_next(pd, pi, p)
        nmd, nmi = minus_next(md, mi, p)
        a, b = plus_next(qpd, qpi, q)
        e, f = minus_next(qmd, qmi, q)
        hold = lambda new, old: jnp.where(late, new, old)
        return npd, npi, nmd, nmi, hold(a, qpd), hold(b, qpi), hold(e, qmd), hold(f, qmi)

    one_ = jnp.int32(1)
    lax.fori_loop(0, slots + 1, step, (
        one_, plus_start(1, p), one_, minus_start(1, p),
        one_, plus_start(1, q), one_, minus_start(1, q)))

    def sent_own(i, carry):
        t = slot(c, i)
        remote(own_rows(i), t, psem.at[t], nxt).wait_send()
        remote(own_rows(i), t, msem.at[t], prv).wait_send()
        remote(own_rows(i), t, dsem.at[t], mate).wait_send()
        return carry

    lax.fori_loop(c, nb, sent_own, 0)

    for d in range(1, CHIPS - 1):
        s = (z + CHIPS - d) % CHIPS
        k = 2 * s + p

        def sent_plus(i, carry):
            t = slot(k, i)
            remote(lv.at[t], t, psem.at[t], nxt).wait_send()
            return carry

        lax.fori_loop(jnp.maximum(k, split(s, d + 1, p)), nb, sent_plus, 0)

        def sent_plus_mate(i, carry):
            t = slot(k, i)
            remote(lv.at[t], t, dsem.at[t], mate).wait_send()
            return carry

        lax.fori_loop(jnp.maximum(k, split(s, d, p)), nb, sent_plus_mate, 0)

        s2 = (z + d) % CHIPS
        k2 = 2 * s2 + p

        def sent_minus(i, carry):
            t = slot(k2, i)
            remote(lv.at[t], t, msem.at[t], prv).wait_send()
            return carry

        lax.fori_loop(k2, split(s2, CHIPS - 1 - d, p), sent_minus, 0)

        def sent_minus_mate(i, carry):
            t = slot(k2, i)
            remote(lv.at[t], t, dsem.at[t], mate).wait_send()
            return carry

        lax.fori_loop(k2, split(s2, CHIPS - d, p), sent_minus_mate, 0)


def solution(mesh):
    def local(l_cols, b_cols):
        order, width = b_cols.shape
        nb = order // BLOCK
        tiles = nb * (nb + 1) // 2
        acc = pl.pallas_call(
            functools.partial(kernel, nb),
            out_shape=pltpu.VMEM((order, width), jnp.float32),
            in_specs=[pl.BlockSpec(memory_space=pltpu.HBM)] * 2,
            out_specs=pl.BlockSpec(memory_space=pltpu.VMEM),
            scratch_shapes=[
                pltpu.VMEM((tiles, BLOCK, BLOCK), jnp.bfloat16),
                pltpu.VMEM((order, width), jnp.bfloat16),
                pltpu.SemaphoreType.DMA((tiles,)),
                pltpu.SemaphoreType.DMA((tiles,)),
                pltpu.SemaphoreType.DMA((tiles,)),
                pltpu.SemaphoreType.DMA((tiles,)),
                pltpu.SemaphoreType.DMA((nb,)),
            ],
            compiler_params=pltpu.CompilerParams(
                collective_id=0, has_side_effects=True, vmem_limit_bytes=34 * 2**20),
        )(l_cols, b_cols)
        return acc.astype(jnp.bfloat16)

    return jax.shard_map(local, mesh=mesh, in_specs=(P("batch", "col"), P("batch", "col")),
                         out_specs=P("batch", "col"), check_vma=False)
```

```python
import functools

import jax
import jax.numpy as jnp
from jax import lax
from jax.experimental import pallas as pl
from jax.experimental.pallas import tpu as pltpu
from jax.sharding import PartitionSpec as P

BLOCK = 256
MESH = pl.DeviceIdType.MESH
CHIPS = 8
PLUS_HOPS = (2, 2, 3, 5, 4, 4, 3, 2)
LONGER = {(0, 3): 12, (1, 3): 7, (1, 4): 13, (2, 4): 6, (2, 5): 9}
MORE_ODD = (2, 5)
SLOTS = 36
OWN_SENT = 20


def pick(index, values):
    out = jnp.int32(values[-1])
    for j in range(len(values) - 2, -1, -1):
        out = jnp.where(index == j, jnp.int32(values[j]), out)
    return out


def kernel(nb, l_ref, b_ref, acc, lv, dg, bv, rsem, psem, msem, dsem, bsem):
    c = lax.axis_index("col")
    z, p = c // 2, c % 2
    q = 1 - p
    nxt = ((z + 1) % CHIPS) * 2 + p
    prv = ((z + CHIPS - 1) % CHIPS) * 2 + p
    mate = z * 2 + q
    half = BLOCK // 2

    def split(s, d, par):
        t = jnp.where(d <= pick(s, PLUS_HOPS), 0, nb)
        for (s0, d0), v in LONGER.items():
            v = v - par if (s0, d0) == MORE_ODD else v
            t = jnp.where(s * CHIPS + d == s0 * CHIPS + d0, v, t)
        return t

    def slot(k, i):
        return nb * k - k * (k - 1) // 2 + i - k

    def each(k, i, fn):
        t = slot(k, i)

        @pl.when(i == k)
        def _():
            fn(dg.at[k], t)

        @pl.when(i != k)
        def _():
            fn(lv.at[t], t)

    def remote(ref, t, sem, dev):
        return pltpu.make_async_remote_copy(
            src_ref=ref, dst_ref=ref, send_sem=sem.at[t], recv_sem=rsem.at[t],
            device_id={"col": dev}, device_id_type=MESH)

    def send(k, i, *ways):
        def go(ref, t):
            for sem, dev in ways:
                remote(ref, t, sem, dev).start()
        each(k, i, go)

    def sent(k, i, *ways):
        def go(ref, t):
            for sem, dev in ways:
                remote(ref, t, sem, dev).wait_send()
        each(k, i, go)

    def land(k, i):
        each(k, i, lambda ref, t: remote(ref, t, psem, nxt).wait_recv())

    def b_copy(k):
        rows = pl.ds(pl.multiple_of(k * BLOCK, BLOCK), BLOCK)
        return pltpu.make_async_copy(b_ref.at[rows, :], bv.at[rows, :], bsem.at[k])

    def plus_low(d, par):
        s = (z + CHIPS - d) % CHIPS
        return jnp.maximum(2 * s + par, split(s, d, par))

    def plus_start(d, par):
        return jnp.where(plus_low(d, par) < nb, nb - 1, -1)

    def plus_next(d, i, par):
        more = i > plus_low(d, par)
        ended = i < 0
        i2 = jnp.where(more, i - 1, plus_start(d + 1, par))
        return jnp.where(more | ended, d, d + 1), jnp.where(ended, i, i2)

    def minus_start(d, par):
        s = (z + d) % CHIPS
        k = 2 * s + par
        return jnp.where(split(s, CHIPS - d, par) > k, k, -1)

    def minus_next(d, i, par):
        s = (z + d) % CHIPS
        more = i + 1 < split(s, CHIPS - d, par)
        ended = i < 0
        i2 = jnp.where(more, i + 1, minus_start(d + 1, par))
        return jnp.where(more | ended, d, d + 1), jnp.where(ended, i, i2)

    def plus_block(d, par):
        return 2 * ((z + CHIPS - d) % CHIPS) + par

    def minus_block(d, par):
        return 2 * ((z + d) % CHIPS) + par

    def plus_onward(d, i):
        return (i >= 0) & (split((z + CHIPS - d) % CHIPS, d + 1, p) <= i)

    def minus_onward(d, i):
        return (i >= 0) & (split((z + d) % CHIPS, CHIPS - 1 - d, p) > i)

    barrier = pltpu.get_barrier_semaphore()
    for dev in (nxt, prv, mate):
        pl.semaphore_signal(barrier, inc=1, device_id={"col": dev}, device_id_type=MESH)

    diag_row = pl.multiple_of(c * BLOCK, BLOCK)
    t_diag = slot(c, c)
    pltpu.make_async_copy(
        l_ref.at[pl.ds(diag_row, BLOCK), pl.ds(0, half)],
        dg.at[c, pl.ds(0, BLOCK), :], rsem.at[t_diag]).start()
    pltpu.make_async_copy(
        l_ref.at[pl.ds(diag_row + half, half), pl.ds(half, half)],
        dg.at[c, pl.ds(BLOCK, half), :], rsem.at[t_diag]).start()

    def own_copy(i):
        rows = pl.ds(pl.multiple_of(i * BLOCK, BLOCK), BLOCK)
        t = slot(c, i)
        return pltpu.make_async_copy(l_ref.at[rows, :], lv.at[t], rsem.at[t])

    lax.fori_loop(c + 1, nb, lambda i, x: (own_copy(i).start(), x)[1], 0)
    lax.fori_loop(0, nb, lambda k, x: (b_copy(k).start(), x)[1], 0)
    lax.fori_loop(c, nb, lambda i, x: (land(c, i), x)[1], 0)
    pl.semaphore_wait(barrier, 3)

    def send_own(j, carry):
        send(c, nb - 1 - j, (psem, nxt))
        send(c, c + j, (msem, prv), (dsem, mate))
        return carry

    lax.fori_loop(0, nb - c, send_own, 0)

    def clear(i, carry):
        acc[pl.ds(pl.multiple_of(i * 64, 64), 64), :] = jnp.zeros((64, acc.shape[1]), jnp.float32)
        return carry

    lax.fori_loop(0, acc.shape[0] // 64, clear, 0)
    lax.fori_loop(0, nb, lambda k, x: (b_copy(k).wait(), x)[1], 0)

    width = acc.shape[1] // 2

    def multiply(k, i):
        row = pl.multiple_of(i * BLOCK, BLOCK)
        depth = pl.multiple_of(k * BLOCK, BLOCK)

        @pl.when(i != k)
        def _():
            tile = lv[slot(k, i)]
            for n in range(2):
                cols = slice(n * width, (n + 1) * width)
                acc[pl.ds(row, BLOCK), cols] += jnp.dot(
                    tile, bv[pl.ds(depth, BLOCK), cols], preferred_element_type=jnp.float32)

        @pl.when(i == k)
        def _():
            left, corner = dg[k, :BLOCK, :], dg[k, BLOCK:, :]
            for n in range(2):
                cols = slice(n * width, (n + 1) * width)
                acc[pl.ds(row, BLOCK), cols] += jnp.dot(
                    left, bv[pl.ds(depth, half), cols], preferred_element_type=jnp.float32)
                acc[pl.ds(row + half, half), cols] += jnp.dot(
                    corner, bv[pl.ds(depth + half, half), cols], preferred_element_type=jnp.float32)

    lag = nb - c + 3

    def left_onward(cur):
        pd, pi, md, mi = cur

        @pl.when(plus_onward(pd, pi))
        def _():
            sent(plus_block(pd, p), pi, (psem, nxt))

        @pl.when(minus_onward(md, mi))
        def _():
            sent(minus_block(md, p), mi, (msem, prv))

        return (*plus_next(pd, pi, p), *minus_next(md, mi, p))

    def step(n, cur):
        pd, pi, md, mi, qpd, qpi, qmd, qmi, *old = cur
        pk, mk = plus_block(pd, p), minus_block(md, p)

        @pl.when(pi >= 0)
        def _():
            land(pk, pi)

            @pl.when(plus_onward(pd, pi))
            def _():
                send(pk, pi, (psem, nxt))

            send(pk, pi, (dsem, mate))

        @pl.when(mi >= 0)
        def _():
            land(mk, mi)

            @pl.when(minus_onward(md, mi))
            def _():
                send(mk, mi, (msem, prv))

            send(mk, mi, (dsem, mate))

        late = n >= 1
        own = jnp.where(c + n < nb, c + n, -1)
        other = jnp.where(mate + n < nb, mate + n, -1)
        ks = (pk, mk, c, plus_block(qpd, q), minus_block(qmd, q), mate)
        is_ = (pi, mi, own, jnp.where(late, qpi, -1), jnp.where(late, qmi, -1), other)

        def one(j, carry):
            k, i = ks[-1], is_[-1]
            for x in range(4, -1, -1):
                k = jnp.where(j == x, ks[x], k)
                i = jnp.where(j == x, is_[x], i)

            @pl.when(i >= 0)
            def _():
                @pl.when(j >= 3)
                def _():
                    land(k, i)

                multiply(k, i)

                @pl.when(j < 3)
                def _():
                    sent(k, i, (dsem, mate))

            return carry

        lax.fori_loop(0, 6, one, 0)

        gone = c + n - OWN_SENT

        @pl.when((n >= OWN_SENT) & (gone < nb))
        def _():
            sent(c, gone, (psem, nxt), (msem, prv))

        npd, npi = plus_next(pd, pi, p)
        nmd, nmi = minus_next(md, mi, p)
        a, b = plus_next(qpd, qpi, q)
        e, f = minus_next(qmd, qmi, q)
        hold = lambda new, was: jnp.where(late, new, was)
        again = n >= lag
        stay = jnp.int32(-1)
        view = [jnp.where(again, x, y) for x, y in zip(old, (old[0], stay, old[2], stay))]
        moved = left_onward(view)
        old = [jnp.where(again, x, y) for x, y in zip(moved, old)]
        return (npd, npi, nmd, nmi, hold(a, qpd), hold(b, qpi), hold(e, qmd), hold(f, qmi), *old)

    one_ = jnp.int32(1)
    mine = (one_, plus_start(1, p), one_, minus_start(1, p))
    other = (one_, plus_start(1, q), one_, minus_start(1, q))
    state = lax.fori_loop(0, SLOTS, step, (*mine, *other, *mine))
    lax.fori_loop(0, lag, lambda n, cur: left_onward(cur), tuple(state[8:]))


def round_kernel(x_ref, o_ref, buf, sem):
    n = sem.shape[0]
    rows = x_ref.shape[0] // n
    step = 64

    def copy(j):
        part = pl.ds(pl.multiple_of(j * rows, rows), rows)
        return pltpu.make_async_copy(buf.at[part, :], o_ref.at[part, :], sem.at[j])

    def one(j, carry):
        def some(m, carry):
            part = pl.ds(pl.multiple_of(j * rows + m * step, step), step)
            buf[part, :] = x_ref[part, :].astype(buf.dtype)
            return carry

        lax.fori_loop(0, rows // step, some, 0)
        copy(j).start()
        return carry

    lax.fori_loop(0, n, one, 0)
    lax.fori_loop(0, n, lambda j, x: (copy(j).wait(), x)[1], 0)


def solution(mesh):
    def local(l_cols, b_cols):
        order, width = b_cols.shape
        nb = order // BLOCK
        tiles = nb * (nb + 1) // 2
        l_cols = pltpu.with_memory_space_constraint(l_cols, pltpu.HBM)
        b_cols = pltpu.with_memory_space_constraint(b_cols, pltpu.HBM)
        acc = pl.pallas_call(
            functools.partial(kernel, nb),
            out_shape=pltpu.VMEM((order, width), jnp.float32),
            in_specs=[pl.BlockSpec(memory_space=pltpu.HBM)] * 2,
            out_specs=pl.BlockSpec(memory_space=pltpu.VMEM),
            scratch_shapes=[
                pltpu.VMEM((tiles, BLOCK, BLOCK), jnp.bfloat16),
                pltpu.VMEM((nb, BLOCK + BLOCK // 2, BLOCK // 2), jnp.bfloat16),
                pltpu.VMEM((order, width), jnp.bfloat16),
                pltpu.SemaphoreType.DMA((tiles,)),
                pltpu.SemaphoreType.DMA((tiles,)),
                pltpu.SemaphoreType.DMA((tiles,)),
                pltpu.SemaphoreType.DMA((tiles,)),
                pltpu.SemaphoreType.DMA((nb,)),
            ],
            compiler_params=pltpu.CompilerParams(
                collective_id=0, has_side_effects=True, vmem_limit_bytes=34 * 2**20),
        )(l_cols, b_cols)
        return pl.pallas_call(
            round_kernel,
            out_shape=jax.ShapeDtypeStruct((order, width), jnp.bfloat16),
            in_specs=[pl.BlockSpec(memory_space=pltpu.VMEM)],
            out_specs=pl.BlockSpec(memory_space=pltpu.HBM),
            scratch_shapes=[
                pltpu.VMEM((order, width), jnp.bfloat16),
                pltpu.SemaphoreType.DMA((16,)),
            ],
            compiler_params=pltpu.CompilerParams(vmem_limit_bytes=16 * 2**20),
        )(acc)

    return jax.shard_map(local, mesh=mesh, in_specs=(P("batch", "col"), P("batch", "col")),
                         out_specs=P("batch", "col"), check_vma=False)
```

```python
import functools

import jax
import jax.numpy as jnp
from jax import lax
from jax.experimental import pallas as pl
from jax.experimental.pallas import tpu as pltpu
from jax.sharding import PartitionSpec as P

BLOCK = 256
MESH = pl.DeviceIdType.MESH
CHIPS = 8
PLUS_HOPS = (2, 2, 3, 5, 4, 4, 3, 2)
LONGER = {(0, 3): 12, (1, 3): 7, (1, 4): 13, (2, 4): 6, (2, 5): 9}
MORE_ODD = (2, 5)
SLOTS = 36
OWN_SENT = 20


def pick(index, values):
    out = jnp.int32(values[-1])
    for j in range(len(values) - 2, -1, -1):
        out = jnp.where(index == j, jnp.int32(values[j]), out)
    return out


def kernel(nb, l_ref, b_ref, acc, lv, dg, bv, rsem, psem, msem, dsem, bsem):
    c = lax.axis_index("col")
    z, p = c // 2, c % 2
    q = 1 - p
    nxt = ((z + 1) % CHIPS) * 2 + p
    prv = ((z + CHIPS - 1) % CHIPS) * 2 + p
    mate = z * 2 + q
    half = BLOCK // 2

    def split(s, d, par):
        t = jnp.where(d <= pick(s, PLUS_HOPS), 0, nb)
        for (s0, d0), v in LONGER.items():
            v = v - par if (s0, d0) == MORE_ODD else v
            t = jnp.where(s * CHIPS + d == s0 * CHIPS + d0, v, t)
        return t

    def slot(k, i):
        return nb * k - k * (k - 1) // 2 + i - k

    def each(k, i, fn):
        t = slot(k, i)

        @pl.when(i == k)
        def _():
            fn(dg.at[k], t)

        @pl.when(i != k)
        def _():
            fn(lv.at[t], t)

    def remote(ref, t, sem, dev):
        return pltpu.make_async_remote_copy(
            src_ref=ref, dst_ref=ref, send_sem=sem.at[t], recv_sem=rsem.at[t],
            device_id={"col": dev}, device_id_type=MESH)

    def send(k, i, *ways):
        def go(ref, t):
            for sem, dev in ways:
                remote(ref, t, sem, dev).start()
        each(k, i, go)

    def sent(k, i, *ways):
        def go(ref, t):
            for sem, dev in ways:
                remote(ref, t, sem, dev).wait_send()
        each(k, i, go)

    def land(k, i):
        each(k, i, lambda ref, t: remote(ref, t, psem, nxt).wait_recv())

    def b_copy(k):
        rows = pl.ds(pl.multiple_of(k * BLOCK, BLOCK), BLOCK)
        return pltpu.make_async_copy(b_ref.at[rows, :], bv.at[rows, :], bsem.at[k])

    def plus_low(d, par):
        s = (z + CHIPS - d) % CHIPS
        return jnp.maximum(2 * s + par, split(s, d, par))

    def plus_start(d, par):
        return jnp.where(plus_low(d, par) < nb, nb - 1, -1)

    def plus_next(d, i, par):
        more = i > plus_low(d, par)
        ended = i < 0
        i2 = jnp.where(more, i - 1, plus_start(d + 1, par))
        return jnp.where(more | ended, d, d + 1), jnp.where(ended, i, i2)

    def minus_start(d, par):
        s = (z + d) % CHIPS
        k = 2 * s + par
        return jnp.where(split(s, CHIPS - d, par) > k, k, -1)

    def minus_next(d, i, par):
        s = (z + d) % CHIPS
        more = i + 1 < split(s, CHIPS - d, par)
        ended = i < 0
        i2 = jnp.where(more, i + 1, minus_start(d + 1, par))
        return jnp.where(more | ended, d, d + 1), jnp.where(ended, i, i2)

    def plus_block(d, par):
        return 2 * ((z + CHIPS - d) % CHIPS) + par

    def minus_block(d, par):
        return 2 * ((z + d) % CHIPS) + par

    def plus_onward(d, i):
        return (i >= 0) & (split((z + CHIPS - d) % CHIPS, d + 1, p) <= i)

    def minus_onward(d, i):
        return (i >= 0) & (split((z + d) % CHIPS, CHIPS - 1 - d, p) > i)

    barrier = pltpu.get_barrier_semaphore()
    for dev in (nxt, prv, mate):
        pl.semaphore_signal(barrier, inc=1, device_id={"col": dev}, device_id_type=MESH)

    diag_row = pl.multiple_of(c * BLOCK, BLOCK)
    t_diag = slot(c, c)
    pltpu.make_async_copy(
        l_ref.at[pl.ds(diag_row, BLOCK), pl.ds(0, half)],
        dg.at[c, pl.ds(0, BLOCK), :], rsem.at[t_diag]).start()
    pltpu.make_async_copy(
        l_ref.at[pl.ds(diag_row + half, half), pl.ds(half, half)],
        dg.at[c, pl.ds(BLOCK, half), :], rsem.at[t_diag]).start()

    def own_copy(i):
        rows = pl.ds(pl.multiple_of(i * BLOCK, BLOCK), BLOCK)
        t = slot(c, i)
        return pltpu.make_async_copy(l_ref.at[rows, :], lv.at[t], rsem.at[t])

    lax.fori_loop(c + 1, nb, lambda i, x: (own_copy(i).start(), x)[1], 0)
    lax.fori_loop(c, nb, lambda i, x: (land(c, i), x)[1], 0)
    pl.semaphore_wait(barrier, 3)

    def send_own(j, carry):
        send(c, nb - 1 - j, (psem, nxt))
        send(c, c + j, (msem, prv), (dsem, mate))
        return carry

    lax.fori_loop(0, nb - c, send_own, 0)
    lax.fori_loop(0, nb, lambda k, x: (b_copy(k).start(), x)[1], 0)

    def clear(i, carry):
        acc[pl.ds(pl.multiple_of(i * 64, 64), 64), :] = jnp.zeros((64, acc.shape[1]), jnp.float32)
        return carry

    lax.fori_loop(0, acc.shape[0] // 64, clear, 0)
    lax.fori_loop(0, nb, lambda k, x: (b_copy(k).wait(), x)[1], 0)

    width = acc.shape[1] // 2

    def multiply(k, i):
        row = pl.multiple_of(i * BLOCK, BLOCK)
        depth = pl.multiple_of(k * BLOCK, BLOCK)

        @pl.when(i != k)
        def _():
            tile = lv[slot(k, i)]
            for n in range(2):
                cols = slice(n * width, (n + 1) * width)
                acc[pl.ds(row, BLOCK), cols] += jnp.dot(
                    tile, bv[pl.ds(depth, BLOCK), cols], preferred_element_type=jnp.float32)

        @pl.when(i == k)
        def _():
            left, corner = dg[k, :BLOCK, :], dg[k, BLOCK:, :]
            for n in range(2):
                cols = slice(n * width, (n + 1) * width)
                acc[pl.ds(row, BLOCK), cols] += jnp.dot(
                    left, bv[pl.ds(depth, half), cols], preferred_element_type=jnp.float32)
                acc[pl.ds(row + half, half), cols] += jnp.dot(
                    corner, bv[pl.ds(depth + half, half), cols], preferred_element_type=jnp.float32)

    lag = nb - c + 3

    def left_onward(cur):
        pd, pi, md, mi = cur

        @pl.when(plus_onward(pd, pi))
        def _():
            sent(plus_block(pd, p), pi, (psem, nxt))

        @pl.when(minus_onward(md, mi))
        def _():
            sent(minus_block(md, p), mi, (msem, prv))

        return (*plus_next(pd, pi, p), *minus_next(md, mi, p))

    def step(n, cur):
        pd, pi, md, mi, qpd, qpi, qmd, qmi, *old = cur
        pk, mk = plus_block(pd, p), minus_block(md, p)

        @pl.when(pi >= 0)
        def _():
            land(pk, pi)

            @pl.when(plus_onward(pd, pi))
            def _():
                send(pk, pi, (psem, nxt))

            send(pk, pi, (dsem, mate))

        @pl.when(mi >= 0)
        def _():
            land(mk, mi)

            @pl.when(minus_onward(md, mi))
            def _():
                send(mk, mi, (msem, prv))

            send(mk, mi, (dsem, mate))

        late = n >= 1
        own = jnp.where(c + n < nb, c + n, -1)
        other = jnp.where(mate + n < nb, mate + n, -1)
        ks = (pk, mk, c, plus_block(qpd, q), minus_block(qmd, q), mate)
        is_ = (pi, mi, own, jnp.where(late, qpi, -1), jnp.where(late, qmi, -1), other)

        def one(j, carry):
            k, i = ks[-1], is_[-1]
            for x in range(4, -1, -1):
                k = jnp.where(j == x, ks[x], k)
                i = jnp.where(j == x, is_[x], i)

            @pl.when(i >= 0)
            def _():
                @pl.when(j >= 3)
                def _():
                    land(k, i)

                multiply(k, i)

            return carry

        lax.fori_loop(0, 6, one, 0)

        for k, i in zip(ks[:3], is_[:3]):
            @pl.when(i >= 0)
            def _():
                sent(k, i, (dsem, mate))

        gone = c + n - OWN_SENT

        @pl.when((n >= OWN_SENT) & (gone < nb))
        def _():
            sent(c, gone, (psem, nxt), (msem, prv))

        npd, npi = plus_next(pd, pi, p)
        nmd, nmi = minus_next(md, mi, p)
        a, b = plus_next(qpd, qpi, q)
        e, f = minus_next(qmd, qmi, q)
        hold = lambda new, was: jnp.where(late, new, was)
        again = n >= lag
        stay = jnp.int32(-1)
        view = [jnp.where(again, x, y) for x, y in zip(old, (old[0], stay, old[2], stay))]
        moved = left_onward(view)
        old = [jnp.where(again, x, y) for x, y in zip(moved, old)]
        return (npd, npi, nmd, nmi, hold(a, qpd), hold(b, qpi), hold(e, qmd), hold(f, qmi), *old)

    one_ = jnp.int32(1)
    mine = (one_, plus_start(1, p), one_, minus_start(1, p))
    other = (one_, plus_start(1, q), one_, minus_start(1, q))
    state = lax.fori_loop(0, SLOTS, step, (*mine, *other, *mine))
    lax.fori_loop(0, lag, lambda n, cur: left_onward(cur), tuple(state[8:]))


def round_kernel(x_ref, o_ref, buf, sem):
    n = sem.shape[0]
    rows = x_ref.shape[0] // n
    step = 64

    def copy(j):
        part = pl.ds(pl.multiple_of(j * rows, rows), rows)
        return pltpu.make_async_copy(buf.at[part, :], o_ref.at[part, :], sem.at[j])

    def one(j, carry):
        def some(m, carry):
            part = pl.ds(pl.multiple_of(j * rows + m * step, step), step)
            buf[part, :] = x_ref[part, :].astype(buf.dtype)
            return carry

        lax.fori_loop(0, rows // step, some, 0)
        copy(j).start()
        return carry

    lax.fori_loop(0, n, one, 0)
    lax.fori_loop(0, n, lambda j, x: (copy(j).wait(), x)[1], 0)


def solution(mesh):
    def local(l_cols, b_cols):
        order, width = b_cols.shape
        nb = order // BLOCK
        tiles = nb * (nb + 1) // 2
        l_cols = pltpu.with_memory_space_constraint(l_cols, pltpu.HBM)
        b_cols = pltpu.with_memory_space_constraint(b_cols, pltpu.HBM)
        acc = pl.pallas_call(
            functools.partial(kernel, nb),
            out_shape=pltpu.VMEM((order, width), jnp.float32),
            in_specs=[pl.BlockSpec(memory_space=pltpu.HBM)] * 2,
            out_specs=pl.BlockSpec(memory_space=pltpu.VMEM),
            scratch_shapes=[
                pltpu.VMEM((tiles, BLOCK, BLOCK), jnp.bfloat16),
                pltpu.VMEM((nb, BLOCK + BLOCK // 2, BLOCK // 2), jnp.bfloat16),
                pltpu.VMEM((order, width), jnp.bfloat16),
                pltpu.SemaphoreType.DMA((tiles,)),
                pltpu.SemaphoreType.DMA((tiles,)),
                pltpu.SemaphoreType.DMA((tiles,)),
                pltpu.SemaphoreType.DMA((tiles,)),
                pltpu.SemaphoreType.DMA((nb,)),
            ],
            compiler_params=pltpu.CompilerParams(
                collective_id=0, has_side_effects=True, vmem_limit_bytes=34 * 2**20),
        )(l_cols, b_cols)
        return pl.pallas_call(
            round_kernel,
            out_shape=jax.ShapeDtypeStruct((order, width), jnp.bfloat16),
            in_specs=[pl.BlockSpec(memory_space=pltpu.VMEM)],
            out_specs=pl.BlockSpec(memory_space=pltpu.HBM),
            scratch_shapes=[
                pltpu.VMEM((order, width), jnp.bfloat16),
                pltpu.SemaphoreType.DMA((16,)),
            ],
            compiler_params=pltpu.CompilerParams(vmem_limit_bytes=16 * 2**20),
        )(acc)

    return jax.shard_map(local, mesh=mesh, in_specs=(P("batch", "col"), P("batch", "col")),
                         out_specs=P("batch", "col"), check_vma=False)
```

```python
import functools

import jax
import jax.numpy as jnp
from jax import lax
from jax.experimental import pallas as pl
from jax.experimental.pallas import tpu as pltpu
from jax.sharding import PartitionSpec as P

BLOCK = 256
MESH = pl.DeviceIdType.MESH
CHIPS = 8
PLUS_HOPS = (2, 2, 3, 5, 4, 4, 3, 2)
LONGER = {(0, 3): 12, (1, 3): 7, (1, 4): 13, (2, 4): 6, (2, 5): 9}
MORE_ODD = (2, 5)
SLOTS = 37
FIRST_SENT = 20


def pick(index, values):
    out = jnp.int32(values[-1])
    for j in range(len(values) - 2, -1, -1):
        out = jnp.where(index == j, jnp.int32(values[j]), out)
    return out


def kernel(nb, l_ref, b_ref, acc, lv, dg, bv, rsem, fsem, dsem, bsem):
    c = lax.axis_index("col")
    z, p = c // 2, c % 2
    q = 1 - p
    mate = z * 2 + q
    ahead = ((z + CHIPS + 2 * p - 1) % CHIPS) * 2 + p
    behind = ((z + CHIPS + 1 - 2 * p) % CHIPS) * 2 + p
    half = BLOCK // 2

    def split(s, d, par):
        t = jnp.where(d <= pick(s, PLUS_HOPS), 0, nb)
        for (s0, d0), v in LONGER.items():
            v = v - par if (s0, d0) == MORE_ODD else v
            t = jnp.where(s * CHIPS + d == s0 * CHIPS + d0, v, t)
        return t

    def source(core, d):
        return (z + CHIPS + (1 - 2 * core) * d) % CHIPS

    def bounds(core, d, par):
        s = source(core, d)
        k = 2 * s + par
        plus = core == 1
        here = split(s, jnp.where(plus, d, CHIPS - d), par)
        on = split(s, jnp.where(plus, d + 1, CHIPS - 1 - d), par)
        low = jnp.where(plus, jnp.maximum(k, here), k)
        high = jnp.where(plus, nb, here)
        on_low = jnp.where(plus, jnp.maximum(k, on), k)
        on_high = jnp.where(plus, nb, on)
        return k, low, high, on_low, on_high

    def inside(i, low, high):
        return (i >= low) & (i < high)

    def ends(core, d):
        _, l0, h0, _, _ = bounds(core, d, 0)
        _, l1, h1, _, _ = bounds(core, d, 1)
        return jnp.minimum(l0, l1), jnp.maximum(h0, h1)

    def start(core, d):
        low, high = ends(core, d)
        return jnp.where(low < high, jnp.where(core == 1, high - 1, low), -1)

    def advance(core, d, i):
        low, high = ends(core, d)
        j = jnp.where(core == 1, i - 1, i + 1)
        more = inside(j, low, high)
        ended = i < 0
        j = jnp.where(more, j, start(core, d + 1))
        return jnp.where(more | ended, d, d + 1), jnp.where(ended, i, j)

    def tiles(core, d, i):
        out = []
        for par in range(2):
            k, low, high, on_low, on_high = bounds(core, d, par)
            out.append((k, jnp.where(inside(i, low, high), i, -1), inside(i, on_low, on_high)))
        return out

    def slot(k, i):
        return nb * k - k * (k - 1) // 2 + i - k

    def each(k, i, fn):
        t = slot(k, i)

        @pl.when(i == k)
        def _():
            fn(dg.at[k], t)

        @pl.when(i != k)
        def _():
            fn(lv.at[t], t)

    def remote(ref, t, sem, dev):
        return pltpu.make_async_remote_copy(
            src_ref=ref, dst_ref=ref, send_sem=sem.at[t], recv_sem=rsem.at[t],
            device_id={"col": dev}, device_id_type=MESH)

    def send(k, i, sem, dev):
        each(k, i, lambda ref, t: remote(ref, t, sem, dev).start())

    def sent(k, i, sem, dev):
        each(k, i, lambda ref, t: remote(ref, t, sem, dev).wait_send())

    def land(k, i):
        each(k, i, lambda ref, t: remote(ref, t, fsem, ahead).wait_recv())

    def b_copy(k):
        rows = pl.ds(pl.multiple_of(k * BLOCK, BLOCK), BLOCK)
        return pltpu.make_async_copy(b_ref.at[rows, :], bv.at[rows, :], bsem.at[k])

    barrier = pltpu.get_barrier_semaphore()
    for dev in (ahead, behind, mate):
        pl.semaphore_signal(barrier, inc=1, device_id={"col": dev}, device_id_type=MESH)

    diag_row = pl.multiple_of(c * BLOCK, BLOCK)
    t_diag = slot(c, c)
    pltpu.make_async_copy(
        l_ref.at[pl.ds(diag_row, BLOCK), pl.ds(0, half)],
        dg.at[c, pl.ds(0, BLOCK), :], rsem.at[t_diag]).start()
    pltpu.make_async_copy(
        l_ref.at[pl.ds(diag_row + half, half), pl.ds(half, half)],
        dg.at[c, pl.ds(BLOCK, half), :], rsem.at[t_diag]).start()

    def own_copy(i):
        rows = pl.ds(pl.multiple_of(i * BLOCK, BLOCK), BLOCK)
        t = slot(c, i)
        return pltpu.make_async_copy(l_ref.at[rows, :], lv.at[t], rsem.at[t])

    lax.fori_loop(c + 1, nb, lambda i, x: (own_copy(i).start(), x)[1], 0)
    lax.fori_loop(c, nb, lambda i, x: (land(c, i), x)[1], 0)
    pl.semaphore_wait(barrier, 3)

    lax.fori_loop(0, nb - c, lambda j, x: (
        send(c, jnp.where(p == 1, c + j, nb - 1 - j), dsem, mate), x)[1], 0)
    lax.fori_loop(0, nb, lambda k, x: (b_copy(k).start(), x)[1], 0)

    def send_first(j, carry):
        i = jnp.where(p == 1, nb - 1 - j, 2 * z + j)

        @pl.when(i >= c)
        def _():
            send(c, i, fsem, ahead)

        @pl.when(i >= mate)
        def _():
            land(mate, i)
            send(mate, i, fsem, ahead)

        return carry

    lax.fori_loop(0, nb - 2 * z, send_first, 0)

    def clear(i, carry):
        acc[pl.ds(pl.multiple_of(i * 64, 64), 64), :] = jnp.zeros((64, acc.shape[1]), jnp.float32)
        return carry

    lax.fori_loop(0, acc.shape[0] // 64, clear, 0)
    lax.fori_loop(0, nb, lambda k, x: (b_copy(k).wait(), x)[1], 0)

    width = acc.shape[1] // 2

    def multiply(k, i):
        row = pl.multiple_of(i * BLOCK, BLOCK)
        depth = pl.multiple_of(k * BLOCK, BLOCK)

        @pl.when(i != k)
        def _():
            tile = lv[slot(k, i)]
            for n in range(2):
                cols = slice(n * width, (n + 1) * width)
                acc[pl.ds(row, BLOCK), cols] += jnp.dot(
                    tile, bv[pl.ds(depth, BLOCK), cols], preferred_element_type=jnp.float32)

        @pl.when(i == k)
        def _():
            left, corner = dg[k, :BLOCK, :], dg[k, BLOCK:, :]
            for n in range(2):
                cols = slice(n * width, (n + 1) * width)
                acc[pl.ds(row, BLOCK), cols] += jnp.dot(
                    left, bv[pl.ds(depth, half), cols], preferred_element_type=jnp.float32)
                acc[pl.ds(row + half, half), cols] += jnp.dot(
                    corner, bv[pl.ds(depth + half, half), cols], preferred_element_type=jnp.float32)

    lag = nb - 2 * z + 3

    def left_onward(d, i):
        for k, _, on in tiles(p, d, i):
            @pl.when(on)
            def _():
                sent(k, i, fsem, ahead)

        return advance(p, d, i)

    def step(n, cur):
        d, i, qd, qi, od, oi = cur
        mine = tiles(p, d, i)
        for k, r, on in mine:
            @pl.when(r >= 0)
            def _():
                land(k, r)

                @pl.when(on)
                def _():
                    send(k, r, fsem, ahead)

                send(k, r, dsem, mate)

        late = n >= 1
        theirs = tiles(q, qd, jnp.where(late, qi, -1))
        own = jnp.where(c + n < nb, c + n, -1)
        other = jnp.where(mate + n < nb, mate + n, -1)
        todo = [x[:2] for x in mine] + [(c, own), (mate, other)] + [x[:2] for x in theirs]

        def one(j, carry):
            k, r = todo[-1]
            for x in range(4, -1, -1):
                k = jnp.where(j == x, todo[x][0], k)
                r = jnp.where(j == x, todo[x][1], r)

            @pl.when(r >= 0)
            def _():
                @pl.when(j >= 4)
                def _():
                    land(k, r)

                multiply(k, r)

            return carry

        lax.fori_loop(0, 6, one, 0)

        for k, r in todo[:3]:
            @pl.when(r >= 0)
            def _():
                sent(k, r, dsem, mate)

        gone = n - FIRST_SENT
        for k in (c, mate):
            @pl.when((gone >= 0) & (k + gone < nb))
            def _():
                sent(k, k + gone, fsem, ahead)

        nd, ni = advance(p, d, i)
        a, b = advance(q, qd, qi)
        again = n >= lag
        e, f = left_onward(od, jnp.where(again, oi, -1))
        hold = lambda cond, new, was: jnp.where(cond, new, was)
        return nd, ni, hold(late, a, qd), hold(late, b, qi), hold(again, e, od), hold(again, f, oi)

    one_ = jnp.int32(1)
    mine = (one_, start(p, one_))
    state = lax.fori_loop(0, SLOTS, step, (*mine, one_, start(q, one_), *mine))
    lax.fori_loop(0, lag, lambda n, cur: left_onward(*cur), tuple(state[4:]))


def round_kernel(x_ref, o_ref, buf, sem):
    n = sem.shape[0]
    rows = x_ref.shape[0] // n
    step = 64

    def copy(j):
        part = pl.ds(pl.multiple_of(j * rows, rows), rows)
        return pltpu.make_async_copy(buf.at[part, :], o_ref.at[part, :], sem.at[j])

    def one(j, carry):
        def some(m, carry):
            part = pl.ds(pl.multiple_of(j * rows + m * step, step), step)
            buf[part, :] = x_ref[part, :].astype(buf.dtype)
            return carry

        lax.fori_loop(0, rows // step, some, 0)
        copy(j).start()
        return carry

    lax.fori_loop(0, n, one, 0)
    lax.fori_loop(0, n, lambda j, x: (copy(j).wait(), x)[1], 0)


def solution(mesh):
    def local(l_cols, b_cols):
        order, width = b_cols.shape
        nb = order // BLOCK
        tiles = nb * (nb + 1) // 2
        l_cols = pltpu.with_memory_space_constraint(l_cols, pltpu.HBM)
        b_cols = pltpu.with_memory_space_constraint(b_cols, pltpu.HBM)
        acc = pl.pallas_call(
            functools.partial(kernel, nb),
            out_shape=pltpu.VMEM((order, width), jnp.float32),
            in_specs=[pl.BlockSpec(memory_space=pltpu.HBM)] * 2,
            out_specs=pl.BlockSpec(memory_space=pltpu.VMEM),
            scratch_shapes=[
                pltpu.VMEM((tiles, BLOCK, BLOCK), jnp.bfloat16),
                pltpu.VMEM((nb, BLOCK + BLOCK // 2, BLOCK // 2), jnp.bfloat16),
                pltpu.VMEM((order, width), jnp.bfloat16),
                pltpu.SemaphoreType.DMA((tiles,)),
                pltpu.SemaphoreType.DMA((tiles,)),
                pltpu.SemaphoreType.DMA((tiles,)),
                pltpu.SemaphoreType.DMA((nb,)),
            ],
            compiler_params=pltpu.CompilerParams(
                collective_id=0, has_side_effects=True, vmem_limit_bytes=34 * 2**20),
        )(l_cols, b_cols)
        return pl.pallas_call(
            round_kernel,
            out_shape=jax.ShapeDtypeStruct((order, width), jnp.bfloat16),
            in_specs=[pl.BlockSpec(memory_space=pltpu.VMEM)],
            out_specs=pl.BlockSpec(memory_space=pltpu.HBM),
            scratch_shapes=[
                pltpu.VMEM((order, width), jnp.bfloat16),
                pltpu.SemaphoreType.DMA((16,)),
            ],
            compiler_params=pltpu.CompilerParams(vmem_limit_bytes=16 * 2**20),
        )(acc)

    return jax.shard_map(local, mesh=mesh, in_specs=(P("batch", "col"), P("batch", "col")),
                         out_specs=P("batch", "col"), check_vma=False)
```

```python
import functools

import jax
import jax.numpy as jnp
from jax import lax
from jax.experimental import pallas as pl
from jax.experimental.pallas import tpu as pltpu
from jax.sharding import PartitionSpec as P

BLOCK = 256
MESH = pl.DeviceIdType.MESH
CHIPS = 8
PLUS_HOPS = (2, 2, 3, 5, 4, 4, 3, 2)
LONGER = {(0, 3): 12, (1, 3): 7, (1, 4): 13, (2, 4): 6, (2, 5): 9}
MORE_ODD = (2, 5)
SLOTS = 37
FIRST_SENT = 20


def pick(index, values):
    out = jnp.int32(values[-1])
    for j in range(len(values) - 2, -1, -1):
        out = jnp.where(index == j, jnp.int32(values[j]), out)
    return out


def kernel(nb, l_ref, b_ref, acc, lv, dg, raw, bv, rsem, fsem, dsem, bsem, gsem):
    c = lax.axis_index("col")
    z, p = c // 2, c % 2
    q = 1 - p
    mate = z * 2 + q
    ahead = ((z + CHIPS + 2 * p - 1) % CHIPS) * 2 + p
    behind = ((z + CHIPS + 1 - 2 * p) % CHIPS) * 2 + p
    half = BLOCK // 2

    def split(s, d, par):
        t = jnp.where(d <= pick(s, PLUS_HOPS), 0, nb)
        for (s0, d0), v in LONGER.items():
            v = v - par if (s0, d0) == MORE_ODD else v
            t = jnp.where(s * CHIPS + d == s0 * CHIPS + d0, v, t)
        return t

    def source(core, d):
        return (z + CHIPS + (1 - 2 * core) * d) % CHIPS

    def bounds(core, d, par):
        s = source(core, d)
        k = 2 * s + par
        plus = core == 1
        here = split(s, jnp.where(plus, d, CHIPS - d), par)
        on = split(s, jnp.where(plus, d + 1, CHIPS - 1 - d), par)
        low = jnp.where(plus, jnp.maximum(k, here), k)
        high = jnp.where(plus, nb, here)
        on_low = jnp.where(plus, jnp.maximum(k, on), k)
        on_high = jnp.where(plus, nb, on)
        return k, low, high, on_low, on_high

    def inside(i, low, high):
        return (i >= low) & (i < high)

    def ends(core, d):
        _, l0, h0, _, _ = bounds(core, d, 0)
        _, l1, h1, _, _ = bounds(core, d, 1)
        return jnp.minimum(l0, l1), jnp.maximum(h0, h1)

    def start(core, d):
        low, high = ends(core, d)
        return jnp.where(low < high, jnp.where(core == 1, high - 1, low), -1)

    def advance(core, d, i):
        low, high = ends(core, d)
        j = jnp.where(core == 1, i - 1, i + 1)
        more = inside(j, low, high)
        ended = i < 0
        j = jnp.where(more, j, start(core, d + 1))
        return jnp.where(more | ended, d, d + 1), jnp.where(ended, i, j)

    def tiles(core, d, i):
        out = []
        for par in range(2):
            k, low, high, on_low, on_high = bounds(core, d, par)
            out.append((k, jnp.where(inside(i, low, high), i, -1), inside(i, on_low, on_high)))
        return out

    def slot(k, i):
        return nb * k - k * (k - 1) // 2 + i - k

    def each(k, i, fn):
        t = slot(k, i)

        @pl.when(i == k)
        def _():
            fn(dg.at[k], t)

        @pl.when(i != k)
        def _():
            fn(lv.at[t], t)

    def remote(ref, t, sem, dev):
        return pltpu.make_async_remote_copy(
            src_ref=ref, dst_ref=ref, send_sem=sem.at[t], recv_sem=rsem.at[t],
            device_id={"col": dev}, device_id_type=MESH)

    def send(k, i, sem, dev):
        each(k, i, lambda ref, t: remote(ref, t, sem, dev).start())

    def sent(k, i, sem, dev):
        each(k, i, lambda ref, t: remote(ref, t, sem, dev).wait_send())

    def land(k, i):
        each(k, i, lambda ref, t: remote(ref, t, fsem, ahead).wait_recv())

    def b_copy(k):
        rows = pl.ds(pl.multiple_of(k * BLOCK, BLOCK), BLOCK)
        return pltpu.make_async_copy(b_ref.at[rows, :], bv.at[rows, :], bsem.at[k])

    barrier = pltpu.get_barrier_semaphore()
    for dev in (ahead, behind, mate):
        pl.semaphore_signal(barrier, inc=1, device_id={"col": dev}, device_id_type=MESH)

    diag_row = pl.multiple_of(c * BLOCK, BLOCK)
    quarter = [
        pltpu.make_async_copy(l_ref.at[pl.ds(diag_row, half), pl.ds(0, half)], raw.at[0], gsem.at[0]),
        pltpu.make_async_copy(l_ref.at[pl.ds(diag_row + half, half), pl.ds(half, half)], raw.at[1], gsem.at[1]),
        pltpu.make_async_copy(
            l_ref.at[pl.ds(diag_row + half, half), pl.ds(0, half)], dg.at[c, pl.ds(half, half), :], gsem.at[2]),
    ]
    for copy in quarter:
        copy.start()
    row = lax.broadcasted_iota(jnp.int32, (half, half), 0)
    col = lax.broadcasted_iota(jnp.int32, (half, half), 1)

    def own_copy(i):
        rows = pl.ds(pl.multiple_of(i * BLOCK, BLOCK), BLOCK)
        t = slot(c, i)
        return pltpu.make_async_copy(l_ref.at[rows, :], lv.at[t], rsem.at[t])

    lax.fori_loop(c + 1, nb, lambda i, x: (own_copy(i).start(), x)[1], 0)
    for copy in quarter:
        copy.wait()
    corner = raw[1].astype(jnp.float32)
    dg[c, :half, :] = jnp.where(row >= col, raw[0].astype(jnp.float32), corner.T).astype(dg.dtype)
    line = jnp.sum(jnp.where(row == col, corner, 0.0), axis=0, keepdims=True)
    dg[c, BLOCK:, :] = jnp.broadcast_to(line, (dg.shape[1] - BLOCK, half)).astype(dg.dtype)
    lax.fori_loop(c + 1, nb, lambda i, x: (own_copy(i).wait(), x)[1], 0)
    lax.fori_loop(0, nb, lambda k, x: (b_copy(k).start(), x)[1], 0)
    pl.semaphore_wait(barrier, 3)

    send(c, jnp.where(p == 1, nb - 1, c), fsem, ahead)
    lax.fori_loop(0, nb - c, lambda j, x: (
        send(c, jnp.where(p == 1, c + j, nb - 1 - j), dsem, mate), x)[1], 0)

    def send_first(j, carry):
        i = jnp.where(p == 1, nb - 1 - j, 2 * z + j)

        @pl.when((i >= c) & (j > 0))
        def _():
            send(c, i, fsem, ahead)

        @pl.when(i >= mate)
        def _():
            land(mate, i)
            send(mate, i, fsem, ahead)

        return carry

    lax.fori_loop(0, nb - 2 * z, send_first, 0)

    def clear(i, carry):
        acc[pl.ds(pl.multiple_of(i * 64, 64), 64), :] = jnp.zeros((64, acc.shape[1]), jnp.float32)
        return carry

    lax.fori_loop(0, acc.shape[0] // 64, clear, 0)
    lax.fori_loop(0, nb, lambda k, x: (b_copy(k).wait(), x)[1], 0)

    width = acc.shape[1] // 2

    def multiply(k, i):
        at = pl.multiple_of(i * BLOCK, BLOCK)
        depth = pl.multiple_of(k * BLOCK, BLOCK)

        @pl.when(i != k)
        def _():
            tile = lv[slot(k, i)]
            for n in range(2):
                cols = slice(n * width, (n + 1) * width)
                acc[pl.ds(at, BLOCK), cols] += jnp.dot(
                    tile, bv[pl.ds(depth, BLOCK), cols], preferred_element_type=jnp.float32)

        @pl.when(i == k)
        def _():
            both = dg[k, :half, :].astype(jnp.float32)
            line = dg[k, BLOCK:BLOCK + 1, :].astype(jnp.float32)
            top = jnp.where(row >= col, both, 0.0).astype(lv.dtype)
            left = dg[k, half:BLOCK, :]
            corner = jnp.where(row < col, both, jnp.where(row == col, line, 0.0)).T.astype(lv.dtype)
            for n in range(2):
                cols = slice(n * width, (n + 1) * width)
                upper = bv[pl.ds(depth, half), cols]
                lower = bv[pl.ds(depth + half, half), cols]
                acc[pl.ds(at, half), cols] += jnp.dot(top, upper, preferred_element_type=jnp.float32)
                acc[pl.ds(at + half, half), cols] += jnp.dot(
                    left, upper, preferred_element_type=jnp.float32) + jnp.dot(
                    corner, lower, preferred_element_type=jnp.float32)

    lag = nb - 2 * z + 2

    def left_onward(d, i):
        for k, _, on in tiles(p, d, i):
            @pl.when(on)
            def _():
                sent(k, i, fsem, ahead)

        return advance(p, d, i)

    def step(n, cur):
        d, i, qd, qi, od, oi = cur
        mine = tiles(p, d, i)
        for k, r, on in mine:
            @pl.when(r >= 0)
            def _():
                land(k, r)

                @pl.when(on)
                def _():
                    send(k, r, fsem, ahead)

                send(k, r, dsem, mate)

        late = n >= 1
        theirs = tiles(q, qd, jnp.where(late, qi, -1))
        own = jnp.where(c + n < nb, c + n, -1)
        other = jnp.where(mate + n < nb, mate + n, -1)
        todo = [x[:2] for x in mine] + [(c, own), (mate, other)] + [x[:2] for x in theirs]

        def one(j, carry):
            k, r = todo[-1]
            for x in range(4, -1, -1):
                k = jnp.where(j == x, todo[x][0], k)
                r = jnp.where(j == x, todo[x][1], r)

            @pl.when(r >= 0)
            def _():
                @pl.when(j >= 4)
                def _():
                    land(k, r)

                multiply(k, r)

            return carry

        lax.fori_loop(0, 6, one, 0)

        for k, r in todo[:3]:
            @pl.when(r >= 0)
            def _():
                sent(k, r, dsem, mate)

        gone = n - FIRST_SENT
        for k in (c, mate):
            @pl.when((gone >= 0) & (k + gone < nb))
            def _():
                sent(k, k + gone, fsem, ahead)

        nd, ni = advance(p, d, i)
        a, b = advance(q, qd, qi)
        again = n >= lag
        e, f = left_onward(od, jnp.where(again, oi, -1))
        hold = lambda cond, new, was: jnp.where(cond, new, was)
        return nd, ni, hold(late, a, qd), hold(late, b, qi), hold(again, e, od), hold(again, f, oi)

    one_ = jnp.int32(1)
    mine = (one_, start(p, one_))
    state = lax.fori_loop(0, SLOTS, step, (*mine, one_, start(q, one_), *mine))
    lax.fori_loop(0, lag, lambda n, cur: left_onward(*cur), tuple(state[4:]))


def round_kernel(x_ref, o_ref, buf, sem):
    n = sem.shape[0]
    rows = x_ref.shape[0] // n
    step = 64

    def copy(j):
        part = pl.ds(pl.multiple_of(j * rows, rows), rows)
        return pltpu.make_async_copy(buf.at[part, :], o_ref.at[part, :], sem.at[j])

    def one(j, carry):
        def some(m, carry):
            part = pl.ds(pl.multiple_of(j * rows + m * step, step), step)
            buf[part, :] = x_ref[part, :].astype(buf.dtype)
            return carry

        lax.fori_loop(0, rows // step, some, 0)
        copy(j).start()
        return carry

    lax.fori_loop(0, n, one, 0)
    lax.fori_loop(0, n, lambda j, x: (copy(j).wait(), x)[1], 0)


def solution(mesh):
    def local(l_cols, b_cols):
        order, width = b_cols.shape
        nb = order // BLOCK
        tiles = nb * (nb + 1) // 2
        l_cols = pltpu.with_memory_space_constraint(l_cols, pltpu.HBM)
        b_cols = pltpu.with_memory_space_constraint(b_cols, pltpu.HBM)
        acc = pl.pallas_call(
            functools.partial(kernel, nb),
            out_shape=pltpu.VMEM((order, width), jnp.float32),
            in_specs=[pl.BlockSpec(memory_space=pltpu.HBM)] * 2,
            out_specs=pl.BlockSpec(memory_space=pltpu.VMEM),
            scratch_shapes=[
                pltpu.VMEM((tiles, BLOCK, BLOCK), jnp.bfloat16),
                pltpu.VMEM((nb, BLOCK + 16, BLOCK // 2), jnp.bfloat16),
                pltpu.VMEM((2, BLOCK // 2, BLOCK // 2), jnp.bfloat16),
                pltpu.VMEM((order, width), jnp.bfloat16),
                pltpu.SemaphoreType.DMA((tiles,)),
                pltpu.SemaphoreType.DMA((tiles,)),
                pltpu.SemaphoreType.DMA((tiles,)),
                pltpu.SemaphoreType.DMA((nb,)),
                pltpu.SemaphoreType.DMA((3,)),
            ],
            compiler_params=pltpu.CompilerParams(
                collective_id=0, has_side_effects=True, vmem_limit_bytes=34 * 2**20),
        )(l_cols, b_cols)
        return pl.pallas_call(
            round_kernel,
            out_shape=jax.ShapeDtypeStruct((order, width), jnp.bfloat16),
            in_specs=[pl.BlockSpec(memory_space=pltpu.VMEM)],
            out_specs=pl.BlockSpec(memory_space=pltpu.HBM),
            scratch_shapes=[
                pltpu.VMEM((order, width), jnp.bfloat16),
                pltpu.SemaphoreType.DMA((16,)),
            ],
            compiler_params=pltpu.CompilerParams(vmem_limit_bytes=16 * 2**20),
        )(acc)

    return jax.shard_map(local, mesh=mesh, in_specs=(P("batch", "col"), P("batch", "col")),
                         out_specs=P("batch", "col"), check_vma=False)
```

```python
import functools

import jax
import jax.numpy as jnp
from jax import lax
from jax.experimental import pallas as pl
from jax.experimental.pallas import tpu as pltpu
from jax.sharding import PartitionSpec as P

BLOCK = 256
MESH = pl.DeviceIdType.MESH
CHIPS = 8
PLUS_HOPS = (2, 2, 3, 5, 4, 4, 3, 2)
LONGER = {(0, 3): 12, (1, 3): 7, (1, 4): 13, (2, 4): 6, (2, 5): 9}
MORE_ODD = (2, 5)
SLOTS = 36
RING = 19
LAPS = 4


def pick(index, values):
    out = jnp.int32(values[-1])
    for j in range(len(values) - 2, -1, -1):
        out = jnp.where(index == j, jnp.int32(values[j]), out)
    return out


def kernel(nb, l_ref, b_ref, acc, lv, dg, raw, bv, isem, osem, xsem, fsem, dsem, bsem, credit):
    c = lax.axis_index("col")
    z, p = c // 2, c % 2
    q = 1 - p
    mate = z * 2 + q
    ahead = ((z + CHIPS + 1 - 2 * p) % CHIPS) * 2 + p
    behind = ((z + CHIPS + 2 * p - 1) % CHIPS) * 2 + p
    half = BLOCK // 2
    first_slots = nb - 2 * z

    def split(s, d, par):
        t = jnp.where(d <= pick(s, PLUS_HOPS), 0, nb)
        for (s0, d0), v in LONGER.items():
            v = v - par if (s0, d0) == MORE_ODD else v
            t = jnp.where(s * CHIPS + d == s0 * CHIPS + d0, v, t)
        return t

    def source(core, d):
        return (z + CHIPS + (2 * core - 1) * d) % CHIPS

    def bounds(core, d, par):
        s = source(core, d)
        k = 2 * s + par
        plus = core == 0
        here = split(s, jnp.where(plus, d, CHIPS - d), par)
        on = split(s, jnp.where(plus, d + 1, CHIPS - 1 - d), par)
        low = jnp.where(plus, jnp.maximum(k, here), k)
        high = jnp.where(plus, nb, here)
        on_low = jnp.where(plus, jnp.maximum(k, on), k)
        on_high = jnp.where(plus, nb, on)
        return k, low, high, on_low, on_high

    def inside(i, low, high):
        return (i >= low) & (i < high)

    def ends(core, d):
        _, l0, h0, _, _ = bounds(core, d, 0)
        _, l1, h1, _, _ = bounds(core, d, 1)
        return jnp.minimum(l0, l1), jnp.maximum(h0, h1)

    def start(core, d):
        low, high = ends(core, d)
        return jnp.where(low < high, jnp.where(core == 0, high - 1, low), -1)

    def advance(core, d, i):
        low, high = ends(core, d)
        j = jnp.where(core == 0, i - 1, i + 1)
        more = inside(j, low, high)
        ended = i < 0
        j = jnp.where(more, j, start(core, d + 1))
        return jnp.where(more | ended, d, d + 1), jnp.where(ended, i, j)

    def tiles(core, d, i):
        out = []
        for par in range(2):
            k, low, high, on_low, on_high = bounds(core, d, par)
            out.append((k, inside(i, low, high), inside(i, on_low, on_high)))
        return out

    def slot(k, i):
        return nb * k - k * (k - 1) // 2 + i - k

    def each(k, i, fn):
        @pl.when(i == k)
        def _():
            fn(dg.at[k])

        @pl.when(i != k)
        def _():
            fn(lv.at[slot(k, i)])

    def remote(ref, out, arrive, dev):
        return pltpu.make_async_remote_copy(
            src_ref=ref, dst_ref=ref, send_sem=out, recv_sem=arrive,
            device_id={"col": dev}, device_id_type=MESH)

    def send(k, i, out, arrive, dev):
        each(k, i, lambda ref: remote(ref, out, arrive, dev).start())

    def sent(k, i, out, dev):
        each(k, i, lambda ref: remote(ref, out, isem.at[0], dev).wait_send())

    def land(k, i, arrive):
        each(k, i, lambda ref: remote(ref, fsem.at[0], arrive, ahead).wait_recv())

    def out_sem(m, par):
        return fsem.at[(m % RING) * 2 + par]

    barrier = pltpu.get_barrier_semaphore()
    for dev in (ahead, behind, mate):
        pl.semaphore_signal(barrier, inc=1, device_id={"col": dev}, device_id_type=MESH)

    diag_row = pl.multiple_of(c * BLOCK, BLOCK)
    quarter = [
        pltpu.make_async_copy(l_ref.at[pl.ds(diag_row, half), pl.ds(0, half)], raw.at[0], fsem.at[0]),
        pltpu.make_async_copy(l_ref.at[pl.ds(diag_row + half, half), pl.ds(half, half)], raw.at[1], fsem.at[1]),
        pltpu.make_async_copy(
            l_ref.at[pl.ds(diag_row + half, half), pl.ds(0, half)], dg.at[c, pl.ds(half, half), :], fsem.at[2]),
    ]
    for copy in quarter:
        copy.start()
    row = lax.broadcasted_iota(jnp.int32, (half, half), 0)
    col = lax.broadcasted_iota(jnp.int32, (half, half), 1)

    def own_copy(i):
        rows = pl.ds(pl.multiple_of(i * BLOCK, BLOCK), BLOCK)
        return pltpu.make_async_copy(l_ref.at[rows, :], lv.at[slot(c, i)], dsem.at[i])

    def b_copy(k):
        rows = pl.ds(pl.multiple_of(k * BLOCK, BLOCK), BLOCK)
        return pltpu.make_async_copy(b_ref.at[rows, :], bv.at[rows, :], bsem)

    lax.fori_loop(c + 1, nb, lambda i, x: (own_copy(i).start(), x)[1], 0)
    for copy in quarter:
        copy.wait()
    corner = raw[1].astype(jnp.float32)
    dg[c, :half, :] = jnp.where(row >= col, raw[0].astype(jnp.float32), corner.T).astype(dg.dtype)
    line = jnp.sum(jnp.where(row == col, corner, 0.0), axis=0, keepdims=True)
    dg[c, BLOCK:, :] = jnp.broadcast_to(line, (dg.shape[1] - BLOCK, half)).astype(dg.dtype)
    lax.fori_loop(c + 1, nb, lambda i, x: (own_copy(i).wait(), x)[1], 0)
    lax.fori_loop(0, nb, lambda k, x: (b_copy(k).start(), x)[1], 0)
    pl.semaphore_wait(barrier, 3)

    head = p
    send(c, jnp.where(p == 0, nb - 1, c), out_sem(head, p), isem.at[head * 2 + p], ahead)
    def to_mate(j, carry):
        i = jnp.where(p == 0, c + j, nb - 1 - j)
        send(c, i, dsem.at[i], osem.at[i], mate)
        return carry

    lax.fori_loop(0, nb - c, to_mate, 0)

    def send_first(j, carry):
        i = jnp.where(p == 0, nb - 1 - j, 2 * z + j)

        @pl.when((i >= c) & (j != head))
        def _():
            send(c, i, out_sem(j, p), isem.at[j * 2 + p], ahead)

        @pl.when(i >= mate)
        def _():
            land(mate, i, osem.at[i])
            send(mate, i, out_sem(j, q), isem.at[j * 2 + q], ahead)

        return carry

    lax.fori_loop(0, first_slots, send_first, 0)

    def clear(i, carry):
        acc[pl.ds(pl.multiple_of(i * 64, 64), 64), :] = jnp.zeros((64, acc.shape[1]), jnp.float32)
        return carry

    lax.fori_loop(0, acc.shape[0] // 64, clear, 0)
    pltpu.make_async_copy(b_ref, bv, bsem).wait()

    width = acc.shape[1] // 2

    def pair(k, i):
        at = pl.multiple_of(i * BLOCK, BLOCK)
        depth = pl.multiple_of(k * BLOCK, BLOCK)
        left, right = lv[slot(k, i)], lv[slot(k + 1, i)]
        for n in range(2):
            cols = slice(n * width, (n + 1) * width)
            acc[pl.ds(at, BLOCK), cols] += jnp.dot(
                left, bv[pl.ds(depth, BLOCK), cols], preferred_element_type=jnp.float32) + jnp.dot(
                right, bv[pl.ds(depth + BLOCK, BLOCK), cols], preferred_element_type=jnp.float32)

    def multiply(k, i):
        at = pl.multiple_of(i * BLOCK, BLOCK)
        depth = pl.multiple_of(k * BLOCK, BLOCK)

        @pl.when(i != k)
        def _():
            tile = lv[slot(k, i)]
            for n in range(2):
                cols = slice(n * width, (n + 1) * width)
                acc[pl.ds(at, BLOCK), cols] += jnp.dot(
                    tile, bv[pl.ds(depth, BLOCK), cols], preferred_element_type=jnp.float32)

        @pl.when(i == k)
        def _():
            both = dg[k, :half, :].astype(jnp.float32)
            line = dg[k, BLOCK:BLOCK + 1, :].astype(jnp.float32)
            top = jnp.where(row >= col, both, 0.0).astype(lv.dtype)
            left = dg[k, half:BLOCK, :]
            corner = jnp.where(row < col, both, jnp.where(row == col, line, 0.0)).T.astype(lv.dtype)
            for n in range(2):
                cols = slice(n * width, (n + 1) * width)
                upper = bv[pl.ds(depth, half), cols]
                lower = bv[pl.ds(depth + half, half), cols]
                acc[pl.ds(at, half), cols] += jnp.dot(top, upper, preferred_element_type=jnp.float32)
                acc[pl.ds(at + half, half), cols] += jnp.dot(
                    left, upper, preferred_element_type=jnp.float32) + jnp.dot(
                    corner, lower, preferred_element_type=jnp.float32)

    def left_onward(m, d, i):
        for par, (k, _, on) in enumerate(tiles(p, d, i)):
            @pl.when(on)
            def _():
                sent(k, i, out_sem(m, par), ahead)

        return advance(p, d, i)

    def step(n, cur):
        d, i, qd, qi, od, oi, gone = cur
        mine = tiles(p, d, i)
        lap = (n % LAPS) * 2

        @pl.when(n >= LAPS)
        def _():
            pl.semaphore_wait(credit, 1)

        for par, (k, here, on) in enumerate(mine):
            @pl.when(here)
            def _():
                land(k, i, isem.at[n * 2 + par])

                @pl.when(on)
                def _():
                    send(k, i, out_sem(first_slots + n, par), isem.at[gone * 2 + par], ahead)

                send(k, i, dsem.at[nb + par], xsem.at[lap + par], mate)

        theirs = tiles(q, qd, qi)
        at_home = 2 * z + n
        home = [(2 * z + par, (at_home >= 2 * z + par) & (at_home < nb)) for par in range(2)]
        groups = (
            (mine[0][0], i, mine[0][1], mine[1][1]),
            (home[0][0], at_home, home[0][1], home[1][1]),
            (theirs[0][0], qi, theirs[0][1], theirs[1][1]),
        )

        def one(j, carry):
            k, r, v0, v1 = (
                jnp.where(j == 0, x, jnp.where(j == 1, y, w))
                for x, y, w in zip(*[(g[0], g[1], g[2].astype(jnp.int32), g[3].astype(jnp.int32)) for g in groups]))
            v0, v1 = v0 > 0, v1 > 0
            for par, v in enumerate((v0, v1)):
                @pl.when(v & (j == 2))
                def _():
                    land(k + par, r, xsem.at[lap + par])

            double = v0 & v1 & (r > k + 1)

            @pl.when(double)
            def _():
                pair(k, r)

            @pl.when(jnp.logical_not(double))
            def _():
                def single(par, carry):
                    @pl.when(jnp.where(par == 0, v0.astype(jnp.int32), v1.astype(jnp.int32)) > 0)
                    def _():
                        multiply(k + par, r)

                    return carry

                lax.fori_loop(0, 2, single, 0)

            return carry

        lax.fori_loop(0, 3, one, 0)

        @pl.when(n < SLOTS - LAPS)
        def _():
            pl.semaphore_signal(credit, inc=1, device_id={"col": mate}, device_id_type=MESH)

        for par, (k, here, _) in enumerate(mine):
            @pl.when(here)
            def _():
                sent(k, i, dsem.at[nb + par], mate)

        @pl.when((at_home >= c) & (at_home < nb))
        def _():
            sent(c, at_home, dsem.at[at_home], mate)

        again = n >= 2
        e, f = left_onward(jnp.maximum(n - 2, 0), od, jnp.where(again, oi, -1))
        gone = gone + (mine[0][2] | mine[1][2]).astype(jnp.int32)
        return (*advance(p, d, i), *advance(q, qd, qi), jnp.where(again, e, od), jnp.where(again, f, oi), gone)

    zero, one_ = jnp.int32(0), jnp.int32(1)
    state = lax.fori_loop(0, SLOTS, step, (
        one_, start(p, one_), one_, start(q, one_), zero, start(p, zero), first_slots))
    od, oi = state[4:6]
    left = zero
    for ahead_d in range(2):
        for par in range(2):
            _, _, _, on_low, on_high = bounds(p, od + ahead_d, par)
            left = jnp.where((oi >= 0) & (on_low < on_high), first_slots + 2, left)
    lax.fori_loop(0, left, lambda m, cur: left_onward(SLOTS - 2 + m, *cur), (od, oi))


def round_kernel(x_ref, o_ref, buf, sem):
    n = sem.shape[0]
    rows = x_ref.shape[0] // n
    step = 64

    def copy(j):
        part = pl.ds(pl.multiple_of(j * rows, rows), rows)
        return pltpu.make_async_copy(buf.at[part, :], o_ref.at[part, :], sem.at[j])

    def one(j, carry):
        def some(m, carry):
            part = pl.ds(pl.multiple_of(j * rows + m * step, step), step)
            buf[part, :] = x_ref[part, :].astype(buf.dtype)
            return carry

        lax.fori_loop(0, rows // step, some, 0)
        copy(j).start()
        return carry

    lax.fori_loop(0, n, one, 0)
    lax.fori_loop(0, n, lambda j, x: (copy(j).wait(), x)[1], 0)


def solution(mesh):
    def local(l_cols, b_cols):
        order, width = b_cols.shape
        nb = order // BLOCK
        tiles = nb * (nb + 1) // 2
        l_cols = pltpu.with_memory_space_constraint(l_cols, pltpu.HBM)
        b_cols = pltpu.with_memory_space_constraint(b_cols, pltpu.HBM)
        acc = pl.pallas_call(
            functools.partial(kernel, nb),
            out_shape=pltpu.VMEM((order, width), jnp.float32),
            in_specs=[pl.BlockSpec(memory_space=pltpu.HBM)] * 2,
            out_specs=pl.BlockSpec(memory_space=pltpu.VMEM),
            scratch_shapes=[
                pltpu.VMEM((tiles, BLOCK, BLOCK), jnp.bfloat16),
                pltpu.VMEM((nb, BLOCK + 16, BLOCK // 2), jnp.bfloat16),
                pltpu.VMEM((2, BLOCK // 2, BLOCK // 2), jnp.bfloat16),
                pltpu.VMEM((order, width), jnp.bfloat16),
                pltpu.SemaphoreType.DMA((2 * SLOTS,)),
                pltpu.SemaphoreType.DMA((nb,)),
                pltpu.SemaphoreType.DMA((2 * LAPS,)),
                pltpu.SemaphoreType.DMA((2 * RING,)),
                pltpu.SemaphoreType.DMA((nb + 2,)),
                pltpu.SemaphoreType.DMA,
                pltpu.SemaphoreType.REGULAR,
            ],
            compiler_params=pltpu.CompilerParams(
                collective_id=0, has_side_effects=True, vmem_limit_bytes=34 * 2**20),
        )(l_cols, b_cols)
        return pl.pallas_call(
            round_kernel,
            out_shape=jax.ShapeDtypeStruct((order, width), jnp.bfloat16),
            in_specs=[pl.BlockSpec(memory_space=pltpu.VMEM)],
            out_specs=pl.BlockSpec(memory_space=pltpu.HBM),
            scratch_shapes=[
                pltpu.VMEM((order, width), jnp.bfloat16),
                pltpu.SemaphoreType.DMA((16,)),
            ],
            compiler_params=pltpu.CompilerParams(vmem_limit_bytes=16 * 2**20),
        )(acc)

    return jax.shard_map(local, mesh=mesh, in_specs=(P("batch", "col"), P("batch", "col")),
                         out_specs=P("batch", "col"), check_vma=False)
```

```python
import functools

import jax
import jax.numpy as jnp
from jax import lax
from jax.experimental import pallas as pl
from jax.experimental.pallas import tpu as pltpu
from jax.sharding import PartitionSpec as P

BLOCK = 256
MESH = pl.DeviceIdType.MESH
CHIPS = 8
PLUS_HOPS = (2, 2, 3, 5, 4, 4, 3, 2)
LONGER = {(0, 3): 12, (1, 3): 7, (1, 4): 13, (2, 4): 6, (2, 5): 8}
UP = 1
SLOTS = 36
RING = 19
LAPS = 4


def pick(index, values):
    out = jnp.int32(values[-1])
    for j in range(len(values) - 2, -1, -1):
        out = jnp.where(index == j, jnp.int32(values[j]), out)
    return out


def kernel(nb, l_ref, b_ref, acc, lv, dg, raw, bv, isem, osem, xsem, fsem, dsem, bsem, credit):
    c = lax.axis_index("col")
    z, p = c // 2, c % 2
    q = 1 - p
    mate = z * 2 + q
    way = 1 - 2 * UP
    ahead = ((z + CHIPS + way * (1 - 2 * p)) % CHIPS) * 2 + p
    behind = ((z + CHIPS - way * (1 - 2 * p)) % CHIPS) * 2 + p
    half = BLOCK // 2
    first_slots = nb - 2 * z

    def split(s, d, par):
        t = jnp.where(d <= pick(s, PLUS_HOPS), 0, nb)
        for (s0, d0), v in LONGER.items():
            t = jnp.where(s * CHIPS + d == s0 * CHIPS + d0, v, t)
        return t

    def source(core, d):
        return (z + CHIPS - way * (1 - 2 * core) * d) % CHIPS

    def bounds(core, d, par):
        s = source(core, d)
        k = 2 * s + par
        plus = core == UP
        here = split(s, jnp.where(plus, d, CHIPS - d), par)
        on = split(s, jnp.where(plus, d + 1, CHIPS - 1 - d), par)
        low = jnp.where(plus, jnp.maximum(k, here), k)
        high = jnp.where(plus, nb, here)
        on_low = jnp.where(plus, jnp.maximum(k, on), k)
        on_high = jnp.where(plus, nb, on)
        return k, low, high, on_low, on_high

    def inside(i, low, high):
        return (i >= low) & (i < high)

    def ends(core, d):
        _, l0, h0, _, _ = bounds(core, d, 0)
        _, l1, h1, _, _ = bounds(core, d, 1)
        return jnp.minimum(l0, l1), jnp.maximum(h0, h1)

    def start(core, d):
        low, high = ends(core, d)
        return jnp.where(low < high, jnp.where(core == UP, high - 1, low), -1)

    def advance(core, d, i):
        low, high = ends(core, d)
        j = jnp.where(core == UP, i - 1, i + 1)
        more = inside(j, low, high)
        ended = i < 0
        j = jnp.where(more, j, start(core, d + 1))
        return jnp.where(more | ended, d, d + 1), jnp.where(ended, i, j)

    def tiles(core, d, i):
        out = []
        for par in range(2):
            k, low, high, on_low, on_high = bounds(core, d, par)
            out.append((k, inside(i, low, high), inside(i, on_low, on_high)))
        return out

    def slot(k, i):
        return nb * k - k * (k - 1) // 2 + i - k

    def each(k, i, fn):
        @pl.when(i == k)
        def _():
            fn(dg.at[k])

        @pl.when(i != k)
        def _():
            fn(lv.at[slot(k, i)])

    def remote(ref, out, arrive, dev):
        return pltpu.make_async_remote_copy(
            src_ref=ref, dst_ref=ref, send_sem=out, recv_sem=arrive,
            device_id={"col": dev}, device_id_type=MESH)

    def send(k, i, out, arrive, dev):
        each(k, i, lambda ref: remote(ref, out, arrive, dev).start())

    def sent(k, i, out, dev):
        each(k, i, lambda ref: remote(ref, out, isem.at[0], dev).wait_send())

    def land(k, i, arrive):
        each(k, i, lambda ref: remote(ref, fsem.at[0], arrive, ahead).wait_recv())

    def out_sem(m, par):
        return fsem.at[(m % RING) * 2 + par]

    barrier = pltpu.get_barrier_semaphore()
    for dev in (behind, mate):
        pl.semaphore_signal(barrier, inc=1, device_id={"col": dev}, device_id_type=MESH)

    diag_row = pl.multiple_of(c * BLOCK, BLOCK)
    quarter = [
        pltpu.make_async_copy(l_ref.at[pl.ds(diag_row, half), pl.ds(0, half)], raw.at[0], fsem.at[0]),
        pltpu.make_async_copy(l_ref.at[pl.ds(diag_row + half, half), pl.ds(half, half)], raw.at[1], fsem.at[1]),
        pltpu.make_async_copy(
            l_ref.at[pl.ds(diag_row + half, half), pl.ds(0, half)], dg.at[c, pl.ds(half, half), :], fsem.at[2]),
    ]
    for copy in quarter:
        copy.start()
    row = lax.broadcasted_iota(jnp.int32, (half, half), 0)
    col = lax.broadcasted_iota(jnp.int32, (half, half), 1)

    def own_copy(i):
        rows = pl.ds(pl.multiple_of(i * BLOCK, BLOCK), BLOCK)
        return pltpu.make_async_copy(l_ref.at[rows, :], lv.at[slot(c, i)], dsem.at[i])

    def b_copy(k):
        rows = pl.ds(pl.multiple_of(k * BLOCK, BLOCK), BLOCK)
        return pltpu.make_async_copy(b_ref.at[rows, :], bv.at[rows, :], bsem)

    lax.fori_loop(c + 1, nb, lambda i, x: (own_copy(i).start(), x)[1], 0)
    for copy in quarter:
        copy.wait()
    corner = raw[1].astype(jnp.float32)
    dg[c, :half, :] = jnp.where(row >= col, raw[0].astype(jnp.float32), corner.T).astype(dg.dtype)
    line = jnp.sum(jnp.where(row == col, corner, 0.0), axis=0, keepdims=True)
    dg[c, BLOCK:, :] = jnp.broadcast_to(line, (dg.shape[1] - BLOCK, half)).astype(dg.dtype)
    lax.fori_loop(c + 1, nb, lambda i, x: (own_copy(i).wait(), x)[1], 0)
    lax.fori_loop(0, nb, lambda k, x: (b_copy(k).start(), x)[1], 0)
    with jax.named_scope('barr'):
        pl.semaphore_wait(barrier, 2)

    head = jnp.where(p == UP, 0, p)
    send(c, jnp.where(p == UP, nb - 1, c), out_sem(head, p), isem.at[head * 2 + p], ahead)
    def to_mate(j, carry):
        i = jnp.where(p == UP, c + j, nb - 1 - j)
        send(c, i, dsem.at[i], osem.at[i], mate)
        return carry

    lax.fori_loop(0, nb - c, to_mate, 0)

    def send_first(j, carry):
        i = jnp.where(p == UP, nb - 1 - j, 2 * z + j)

        @pl.when((i >= c) & (j != head))
        def _():
            send(c, i, out_sem(j, p), isem.at[j * 2 + p], ahead)

        @pl.when(i >= mate)
        def _():
            land(mate, i, osem.at[i])
            send(mate, i, out_sem(j, q), isem.at[j * 2 + q], ahead)

        return carry

    with jax.named_scope('first'):
        lax.fori_loop(0, first_slots, send_first, 0)

    def clear(i, carry):
        acc[pl.ds(pl.multiple_of(i * 64, 64), 64), :] = jnp.zeros((64, acc.shape[1]), jnp.float32)
        return carry

    lax.fori_loop(0, acc.shape[0] // 64, clear, 0)
    with jax.named_scope('bwait'):
        pltpu.make_async_copy(b_ref, bv, bsem).wait()

    width = acc.shape[1] // 2

    def pair(k, i):
        at = pl.multiple_of(i * BLOCK, BLOCK)
        depth = pl.multiple_of(k * BLOCK, BLOCK)
        left, right = lv[slot(k, i)], lv[slot(k + 1, i)]
        for n in range(2):
            cols = slice(n * width, (n + 1) * width)
            acc[pl.ds(at, BLOCK), cols] += jnp.dot(
                left, bv[pl.ds(depth, BLOCK), cols], preferred_element_type=jnp.float32) + jnp.dot(
                right, bv[pl.ds(depth + BLOCK, BLOCK), cols], preferred_element_type=jnp.float32)

    def multiply(k, i):
        at = pl.multiple_of(i * BLOCK, BLOCK)
        depth = pl.multiple_of(k * BLOCK, BLOCK)

        @pl.when(i != k)
        def _():
            tile = lv[slot(k, i)]
            for n in range(2):
                cols = slice(n * width, (n + 1) * width)
                acc[pl.ds(at, BLOCK), cols] += jnp.dot(
                    tile, bv[pl.ds(depth, BLOCK), cols], preferred_element_type=jnp.float32)

        @pl.when(i == k)
        def _():
            both = dg[k, :half, :].astype(jnp.float32)
            line = dg[k, BLOCK:BLOCK + 1, :].astype(jnp.float32)
            top = jnp.where(row >= col, both, 0.0).astype(lv.dtype)
            left = dg[k, half:BLOCK, :]
            corner = jnp.where(row < col, both, jnp.where(row == col, line, 0.0)).T.astype(lv.dtype)
            for n in range(2):
                cols = slice(n * width, (n + 1) * width)
                upper = bv[pl.ds(depth, half), cols]
                lower = bv[pl.ds(depth + half, half), cols]
                acc[pl.ds(at, half), cols] += jnp.dot(top, upper, preferred_element_type=jnp.float32)
                acc[pl.ds(at + half, half), cols] += jnp.dot(
                    left, upper, preferred_element_type=jnp.float32) + jnp.dot(
                    corner, lower, preferred_element_type=jnp.float32)

    def left_onward(m, d, i):
        for par, (k, _, on) in enumerate(tiles(p, d, i)):
            @pl.when(on)
            def _():
                sent(k, i, out_sem(m, par), ahead)

        return advance(p, d, i)

    def step(n, cur):
        d, i, qd, qi, od, oi, gone = cur
        mine = tiles(p, d, i)
        lap = (n % LAPS) * 2

        @pl.when(n >= LAPS)
        def _():
            pl.semaphore_wait(credit, 1)

        for par, (k, here, on) in enumerate(mine):
            @pl.when(here)
            def _():
                with jax.named_scope('land'):
                    land(k, i, isem.at[n * 2 + par])

                @pl.when(on)
                def _():
                    send(k, i, out_sem(first_slots + n, par), isem.at[gone * 2 + par], ahead)

                send(k, i, dsem.at[nb + par], xsem.at[lap + par], mate)

        theirs = tiles(q, qd, qi)
        at_home = 2 * z + n
        home = [(2 * z + par, (at_home >= 2 * z + par) & (at_home < nb)) for par in range(2)]
        groups = (
            (mine[0][0], i, mine[0][1], mine[1][1]),
            (home[0][0], at_home, home[0][1], home[1][1]),
            (theirs[0][0], qi, theirs[0][1], theirs[1][1]),
        )

        def one(j, carry):
            k, r, v0, v1 = (
                jnp.where(j == 0, x, jnp.where(j == 1, y, w))
                for x, y, w in zip(*[(g[0], g[1], g[2].astype(jnp.int32), g[3].astype(jnp.int32)) for g in groups]))
            v0, v1 = v0 > 0, v1 > 0
            for par, v in enumerate((v0, v1)):
                @pl.when(v & (j == 2))
                def _():
                    with jax.named_scope('mland'):
                        land(k + par, r, xsem.at[lap + par])

            double = v0 & v1 & (r > k + 1)

            @pl.when(double)
            def _():
                pair(k, r)

            @pl.when(jnp.logical_not(double))
            def _():
                def single(par, carry):
                    @pl.when(jnp.where(par == 0, v0.astype(jnp.int32), v1.astype(jnp.int32)) > 0)
                    def _():
                        multiply(k + par, r)

                    return carry

                lax.fori_loop(0, 2, single, 0)

            return carry

        with jax.named_scope('work'):
            lax.fori_loop(0, 3, one, 0)

        @pl.when(n < SLOTS - LAPS)
        def _():
            pl.semaphore_signal(credit, inc=1, device_id={"col": mate}, device_id_type=MESH)

        for par, (k, here, _) in enumerate(mine):
            @pl.when(here)
            def _():
                sent(k, i, dsem.at[nb + par], mate)

        @pl.when((at_home >= c) & (at_home < nb))
        def _():
            sent(c, at_home, dsem.at[at_home], mate)

        again = n >= 2
        e, f = left_onward(jnp.maximum(n - 2, 0), od, jnp.where(again, oi, -1))
        gone = gone + (mine[0][2] | mine[1][2]).astype(jnp.int32)
        return (*advance(p, d, i), *advance(q, qd, qi), jnp.where(again, e, od), jnp.where(again, f, oi), gone)

    zero, one_ = jnp.int32(0), jnp.int32(1)
    state = lax.fori_loop(0, SLOTS, step, (
        one_, start(p, one_), one_, start(q, one_), zero, start(p, zero), first_slots))
    od, oi = state[4:6]
    left = zero
    for ahead_d in range(2):
        for par in range(2):
            _, _, _, on_low, on_high = bounds(p, od + ahead_d, par)
            left = jnp.where((oi >= 0) & (on_low < on_high), first_slots + 2, left)
    with jax.named_scope('tail'):
        lax.fori_loop(0, left, lambda m, cur: left_onward(SLOTS - 2 + m, *cur), (od, oi))


def round_kernel(x_ref, o_ref, buf, sem):
    n = sem.shape[0]
    rows = x_ref.shape[0] // n
    step = 64

    def copy(j):
        part = pl.ds(pl.multiple_of(j * rows, rows), rows)
        return pltpu.make_async_copy(buf.at[part, :], o_ref.at[part, :], sem.at[j])

    def one(j, carry):
        def some(m, carry):
            part = pl.ds(pl.multiple_of(j * rows + m * step, step), step)
            buf[part, :] = x_ref[part, :].astype(buf.dtype)
            return carry

        lax.fori_loop(0, rows // step, some, 0)
        copy(j).start()
        return carry

    lax.fori_loop(0, n, one, 0)
    lax.fori_loop(0, n, lambda j, x: (copy(j).wait(), x)[1], 0)


def solution(mesh):
    def local(l_cols, b_cols):
        order, width = b_cols.shape
        nb = order // BLOCK
        tiles = nb * (nb + 1) // 2
        l_cols = pltpu.with_memory_space_constraint(l_cols, pltpu.HBM)
        b_cols = pltpu.with_memory_space_constraint(b_cols, pltpu.HBM)
        acc = pl.pallas_call(
            functools.partial(kernel, nb),
            out_shape=pltpu.VMEM((order, width), jnp.float32),
            in_specs=[pl.BlockSpec(memory_space=pltpu.HBM)] * 2,
            out_specs=pl.BlockSpec(memory_space=pltpu.VMEM),
            scratch_shapes=[
                pltpu.VMEM((tiles, BLOCK, BLOCK), jnp.bfloat16),
                pltpu.VMEM((nb, BLOCK + 16, BLOCK // 2), jnp.bfloat16),
                pltpu.VMEM((2, BLOCK // 2, BLOCK // 2), jnp.bfloat16),
                pltpu.VMEM((order, width), jnp.bfloat16),
                pltpu.SemaphoreType.DMA((2 * SLOTS,)),
                pltpu.SemaphoreType.DMA((nb,)),
                pltpu.SemaphoreType.DMA((2 * LAPS,)),
                pltpu.SemaphoreType.DMA((2 * RING,)),
                pltpu.SemaphoreType.DMA((nb + 2,)),
                pltpu.SemaphoreType.DMA,
                pltpu.SemaphoreType.REGULAR,
            ],
            compiler_params=pltpu.CompilerParams(
                collective_id=0, has_side_effects=True, vmem_limit_bytes=34 * 2**20),
        )(l_cols, b_cols)
        return pl.pallas_call(
            round_kernel,
            out_shape=jax.ShapeDtypeStruct((order, width), jnp.bfloat16),
            in_specs=[pl.BlockSpec(memory_space=pltpu.VMEM)],
            out_specs=pl.BlockSpec(memory_space=pltpu.HBM),
            scratch_shapes=[
                pltpu.VMEM((order, width), jnp.bfloat16),
                pltpu.SemaphoreType.DMA((16,)),
            ],
            compiler_params=pltpu.CompilerParams(vmem_limit_bytes=16 * 2**20),
        )(acc)

    return jax.shard_map(local, mesh=mesh, in_specs=(P("batch", "col"), P("batch", "col")),
                         out_specs=P("batch", "col"), check_vma=False)
```

```python
import functools

import jax
import jax.numpy as jnp
from jax import lax
from jax.experimental import pallas as pl
from jax.experimental.pallas import tpu as pltpu
from jax.sharding import PartitionSpec as P

BLOCK = 256
MESH = pl.DeviceIdType.MESH
CHIPS = 8
PLUS_HOPS = (2, 2, 3, 5, 4, 4, 3, 2)
LONGER = {(0, 3): 12, (1, 3): 7, (1, 4): 13, (2, 4): 6, (2, 5): 8}
UP = 1
SLOTS = 36
RING = 19
LAPS = 8
LATER = 3


def pick(index, values):
    out = jnp.int32(values[-1])
    for j in range(len(values) - 2, -1, -1):
        out = jnp.where(index == j, jnp.int32(values[j]), out)
    return out


def kernel(nb, l_ref, b_ref, acc, lv, dg, raw, bv, isem, osem, xsem, fsem, dsem, bsem, credit):
    c = lax.axis_index("col")
    z, p = c // 2, c % 2
    q = 1 - p
    mate = z * 2 + q
    way = 1 - 2 * UP
    ahead = ((z + CHIPS + way * (1 - 2 * p)) % CHIPS) * 2 + p
    behind = ((z + CHIPS - way * (1 - 2 * p)) % CHIPS) * 2 + p
    half = BLOCK // 2
    first_slots = nb - 2 * z

    def split(s, d, par):
        t = jnp.where(d <= pick(s, PLUS_HOPS), 0, nb)
        for (s0, d0), v in LONGER.items():
            t = jnp.where(s * CHIPS + d == s0 * CHIPS + d0, v, t)
        return t

    def source(core, d):
        return (z + CHIPS - way * (1 - 2 * core) * d) % CHIPS

    def bounds(core, d, par):
        s = source(core, d)
        k = 2 * s + par
        plus = core == UP
        here = split(s, jnp.where(plus, d, CHIPS - d), par)
        on = split(s, jnp.where(plus, d + 1, CHIPS - 1 - d), par)
        low = jnp.where(plus, jnp.maximum(k, here), k)
        high = jnp.where(plus, nb, here)
        on_low = jnp.where(plus, jnp.maximum(k, on), k)
        on_high = jnp.where(plus, nb, on)
        return k, low, high, on_low, on_high

    def inside(i, low, high):
        return (i >= low) & (i < high)

    def ends(core, d):
        _, l0, h0, _, _ = bounds(core, d, 0)
        _, l1, h1, _, _ = bounds(core, d, 1)
        return jnp.minimum(l0, l1), jnp.maximum(h0, h1)

    def start(core, d):
        low, high = ends(core, d)
        return jnp.where(low < high, jnp.where(core == UP, high - 1, low), -1)

    def advance(core, d, i):
        low, high = ends(core, d)
        j = jnp.where(core == UP, i - 1, i + 1)
        more = inside(j, low, high)
        ended = i < 0
        j = jnp.where(more, j, start(core, d + 1))
        return jnp.where(more | ended, d, d + 1), jnp.where(ended, i, j)

    def tiles(core, d, i):
        out = []
        for par in range(2):
            k, low, high, on_low, on_high = bounds(core, d, par)
            out.append((k, inside(i, low, high), inside(i, on_low, on_high)))
        return out

    def slot(k, i):
        return nb * k - k * (k - 1) // 2 + i - k

    def each(k, i, fn):
        @pl.when(i == k)
        def _():
            fn(dg.at[k])

        @pl.when(i != k)
        def _():
            fn(lv.at[slot(k, i)])

    def remote(ref, out, arrive, dev):
        return pltpu.make_async_remote_copy(
            src_ref=ref, dst_ref=ref, send_sem=out, recv_sem=arrive,
            device_id={"col": dev}, device_id_type=MESH)

    def send(k, i, out, arrive, dev):
        each(k, i, lambda ref: remote(ref, out, arrive, dev).start())

    def sent(k, i, out, dev):
        each(k, i, lambda ref: remote(ref, out, isem.at[0], dev).wait_send())

    def land(k, i, arrive):
        each(k, i, lambda ref: remote(ref, fsem.at[0], arrive, ahead).wait_recv())

    def out_sem(m, par):
        return fsem.at[(m % RING) * 2 + par]

    barrier = pltpu.get_barrier_semaphore()
    for dev in (behind, mate):
        pl.semaphore_signal(barrier, inc=1, device_id={"col": dev}, device_id_type=MESH)

    diag_row = pl.multiple_of(c * BLOCK, BLOCK)
    quarter = [
        pltpu.make_async_copy(l_ref.at[pl.ds(diag_row, half), pl.ds(0, half)], raw.at[0], fsem.at[0]),
        pltpu.make_async_copy(l_ref.at[pl.ds(diag_row + half, half), pl.ds(half, half)], raw.at[1], fsem.at[1]),
        pltpu.make_async_copy(
            l_ref.at[pl.ds(diag_row + half, half), pl.ds(0, half)], dg.at[c, pl.ds(half, half), :], fsem.at[2]),
    ]
    for copy in quarter:
        copy.start()
    row = lax.broadcasted_iota(jnp.int32, (half, half), 0)
    col = lax.broadcasted_iota(jnp.int32, (half, half), 1)

    def own_copy(i):
        rows = pl.ds(pl.multiple_of(i * BLOCK, BLOCK), BLOCK)
        return pltpu.make_async_copy(l_ref.at[rows, :], lv.at[slot(c, i)], dsem.at[i])

    def b_copy(k):
        rows = pl.ds(pl.multiple_of(k * BLOCK, BLOCK), BLOCK)
        return pltpu.make_async_copy(b_ref.at[rows, :], bv.at[rows, :], bsem)

    lax.fori_loop(c + 1, nb, lambda i, x: (own_copy(i).start(), x)[1], 0)
    for copy in quarter:
        copy.wait()
    corner = raw[1].astype(jnp.float32)
    dg[c, :half, :] = jnp.where(row >= col, raw[0].astype(jnp.float32), corner.T).astype(dg.dtype)
    line = jnp.sum(jnp.where(row == col, corner, 0.0), axis=0, keepdims=True)
    dg[c, BLOCK:, :] = jnp.broadcast_to(line, (dg.shape[1] - BLOCK, half)).astype(dg.dtype)
    lax.fori_loop(c + 1, nb, lambda i, x: (own_copy(i).wait(), x)[1], 0)
    lax.fori_loop(0, nb, lambda k, x: (b_copy(k).start(), x)[1], 0)
    with jax.named_scope('barr'):
        pl.semaphore_wait(barrier, 2)

    head = jnp.where(p == UP, 0, p)
    send(c, jnp.where(p == UP, nb - 1, c), out_sem(head, p), isem.at[head * 2 + p], ahead)
    def to_mate(j, carry):
        i = jnp.where(p == UP, c + j, nb - 1 - j)
        send(c, i, dsem.at[i], osem.at[i], mate)
        return carry

    lax.fori_loop(0, nb - c, to_mate, 0)

    def send_first(j, carry):
        i = jnp.where(p == UP, nb - 1 - j, 2 * z + j)

        @pl.when((i >= c) & (j != head))
        def _():
            send(c, i, out_sem(j, p), isem.at[j * 2 + p], ahead)

        @pl.when(i >= mate)
        def _():
            land(mate, i, osem.at[i])
            send(mate, i, out_sem(j, q), isem.at[j * 2 + q], ahead)

        return carry

    with jax.named_scope('first'):
        lax.fori_loop(0, first_slots, send_first, 0)

    def clear(i, carry):
        acc[pl.ds(pl.multiple_of(i * 64, 64), 64), :] = jnp.zeros((64, acc.shape[1]), jnp.float32)
        return carry

    lax.fori_loop(0, acc.shape[0] // 64, clear, 0)
    with jax.named_scope('bwait'):
        pltpu.make_async_copy(b_ref, bv, bsem).wait()

    width = acc.shape[1] // 2

    def pair(k, i):
        at = pl.multiple_of(i * BLOCK, BLOCK)
        depth = pl.multiple_of(k * BLOCK, BLOCK)
        left, right = lv[slot(k, i)], lv[slot(k + 1, i)]
        for n in range(2):
            cols = slice(n * width, (n + 1) * width)
            acc[pl.ds(at, BLOCK), cols] += jnp.dot(
                left, bv[pl.ds(depth, BLOCK), cols], preferred_element_type=jnp.float32) + jnp.dot(
                right, bv[pl.ds(depth + BLOCK, BLOCK), cols], preferred_element_type=jnp.float32)

    def multiply(k, i):
        at = pl.multiple_of(i * BLOCK, BLOCK)
        depth = pl.multiple_of(k * BLOCK, BLOCK)

        @pl.when(i != k)
        def _():
            tile = lv[slot(k, i)]
            for n in range(2):
                cols = slice(n * width, (n + 1) * width)
                acc[pl.ds(at, BLOCK), cols] += jnp.dot(
                    tile, bv[pl.ds(depth, BLOCK), cols], preferred_element_type=jnp.float32)

        @pl.when(i == k)
        def _():
            both = dg[k, :half, :].astype(jnp.float32)
            line = dg[k, BLOCK:BLOCK + 1, :].astype(jnp.float32)
            top = jnp.where(row >= col, both, 0.0).astype(lv.dtype)
            left = dg[k, half:BLOCK, :]
            corner = jnp.where(row < col, both, jnp.where(row == col, line, 0.0)).T.astype(lv.dtype)
            for n in range(2):
                cols = slice(n * width, (n + 1) * width)
                upper = bv[pl.ds(depth, half), cols]
                lower = bv[pl.ds(depth + half, half), cols]
                acc[pl.ds(at, half), cols] += jnp.dot(top, upper, preferred_element_type=jnp.float32)
                acc[pl.ds(at + half, half), cols] += jnp.dot(
                    left, upper, preferred_element_type=jnp.float32) + jnp.dot(
                    corner, lower, preferred_element_type=jnp.float32)

    def left_onward(m, d, i):
        for par, (k, _, on) in enumerate(tiles(p, d, i)):
            @pl.when(on)
            def _():
                sent(k, i, out_sem(m, par), ahead)

        return advance(p, d, i)

    def use(k, r, v0, v1, from_mate, lap):
        for par, v in enumerate((v0, v1)):
            @pl.when(v & from_mate)
            def _():
                with jax.named_scope('mland'):
                    land(k + par, r, xsem.at[lap + par])

        double = v0 & v1 & (r > k + 1)

        @pl.when(double)
        def _():
            pair(k, r)

        @pl.when(jnp.logical_not(double))
        def _():
            def single(par, carry):
                @pl.when(jnp.where(par == 0, v0.astype(jnp.int32), v1.astype(jnp.int32)) > 0)
                def _():
                    multiply(k + par, r)

                return carry

            lax.fori_loop(0, 2, single, 0)

    def step(n, cur):
        d, i, qd, qi, od, oi, gone = cur
        mine = tiles(p, d, i)
        lap = (n % LAPS) * 2

        @pl.when(n >= LAPS)
        def _():
            pl.semaphore_wait(credit, 1)

        for par, (k, here, on) in enumerate(mine):
            @pl.when(here)
            def _():
                with jax.named_scope('land'):
                    land(k, i, isem.at[n * 2 + par])

                @pl.when(on)
                def _():
                    send(k, i, out_sem(first_slots + n, par), isem.at[gone * 2 + par], ahead)

                send(k, i, dsem.at[nb + par], xsem.at[lap + par], mate)

        late = n >= LATER
        theirs = tiles(q, qd, jnp.where(late, qi, -1))
        at_home = 2 * z + n
        home = [(2 * z + par, (at_home >= 2 * z + par) & (at_home < nb)) for par in range(2)]
        groups = (
            (mine[0][0], i, mine[0][1], mine[1][1]),
            (home[0][0], at_home, home[0][1], home[1][1]),
            (theirs[0][0], qi, theirs[0][1], theirs[1][1]),
        )
        lap_in = ((n + LAPS - LATER) % LAPS) * 2

        def one(j, carry):
            k, r, v0, v1 = (
                jnp.where(j == 0, x, jnp.where(j == 1, y, w))
                for x, y, w in zip(*[(g[0], g[1], g[2].astype(jnp.int32), g[3].astype(jnp.int32)) for g in groups]))
            use(k, r, v0 > 0, v1 > 0, j == 2, lap_in)
            return carry

        with jax.named_scope('work'):
            lax.fori_loop(0, 3, one, 0)

        @pl.when(late & (n - LATER < SLOTS - LAPS))
        def _():
            pl.semaphore_signal(credit, inc=1, device_id={"col": mate}, device_id_type=MESH)

        for par, (k, here, _) in enumerate(mine):
            @pl.when(here)
            def _():
                sent(k, i, dsem.at[nb + par], mate)

        @pl.when((at_home >= c) & (at_home < nb))
        def _():
            sent(c, at_home, dsem.at[at_home], mate)

        again = n >= 2
        e, f = left_onward(jnp.maximum(n - 2, 0), od, jnp.where(again, oi, -1))
        gone = gone + (mine[0][2] | mine[1][2]).astype(jnp.int32)
        g, h = advance(q, qd, qi)
        return (*advance(p, d, i), jnp.where(late, g, qd), jnp.where(late, h, qi), jnp.where(again, e, od), jnp.where(again, f, oi), gone)

    zero, one_ = jnp.int32(0), jnp.int32(1)
    state = lax.fori_loop(0, SLOTS, step, (
        one_, start(p, one_), one_, start(q, one_), zero, start(p, zero), first_slots))
    qd, qi, od, oi = state[2:6]
    left = zero
    for ahead_d in range(2):
        for par in range(2):
            _, _, _, on_low, on_high = bounds(p, od + ahead_d, par)
            left = jnp.where((oi >= 0) & (on_low < on_high), first_slots + 2, left)
    with jax.named_scope('tail'):
        lax.fori_loop(0, left, lambda m, cur: left_onward(SLOTS - 2 + m, *cur), (od, oi))

    def drain(m, cur):
        qd, qi = cur
        (k, v0, _), (_, v1, _) = tiles(q, qd, qi)
        use(k, qi, v0, v1, m >= 0, (m % LAPS) * 2)
        return advance(q, qd, qi)

    with jax.named_scope('drain'):
        lax.fori_loop(SLOTS - LATER, SLOTS, drain, (qd, qi))


def round_kernel(x_ref, o_ref, buf, sem):
    n = sem.shape[0]
    rows = x_ref.shape[0] // n
    step = 64

    def copy(j):
        part = pl.ds(pl.multiple_of(j * rows, rows), rows)
        return pltpu.make_async_copy(buf.at[part, :], o_ref.at[part, :], sem.at[j])

    def one(j, carry):
        def some(m, carry):
            part = pl.ds(pl.multiple_of(j * rows + m * step, step), step)
            buf[part, :] = x_ref[part, :].astype(buf.dtype)
            return carry

        lax.fori_loop(0, rows // step, some, 0)
        copy(j).start()
        return carry

    lax.fori_loop(0, n, one, 0)
    lax.fori_loop(0, n, lambda j, x: (copy(j).wait(), x)[1], 0)


def solution(mesh):
    def local(l_cols, b_cols):
        order, width = b_cols.shape
        nb = order // BLOCK
        tiles = nb * (nb + 1) // 2
        l_cols = pltpu.with_memory_space_constraint(l_cols, pltpu.HBM)
        b_cols = pltpu.with_memory_space_constraint(b_cols, pltpu.HBM)
        acc = pl.pallas_call(
            functools.partial(kernel, nb),
            out_shape=pltpu.VMEM((order, width), jnp.float32),
            in_specs=[pl.BlockSpec(memory_space=pltpu.HBM)] * 2,
            out_specs=pl.BlockSpec(memory_space=pltpu.VMEM),
            scratch_shapes=[
                pltpu.VMEM((tiles, BLOCK, BLOCK), jnp.bfloat16),
                pltpu.VMEM((nb, BLOCK + 16, BLOCK // 2), jnp.bfloat16),
                pltpu.VMEM((2, BLOCK // 2, BLOCK // 2), jnp.bfloat16),
                pltpu.VMEM((order, width), jnp.bfloat16),
                pltpu.SemaphoreType.DMA((2 * SLOTS,)),
                pltpu.SemaphoreType.DMA((nb,)),
                pltpu.SemaphoreType.DMA((2 * LAPS,)),
                pltpu.SemaphoreType.DMA((2 * RING,)),
                pltpu.SemaphoreType.DMA((nb + 2,)),
                pltpu.SemaphoreType.DMA,
                pltpu.SemaphoreType.REGULAR,
            ],
            compiler_params=pltpu.CompilerParams(
                collective_id=0, has_side_effects=True, vmem_limit_bytes=34 * 2**20),
        )(l_cols, b_cols)
        return pl.pallas_call(
            round_kernel,
            out_shape=jax.ShapeDtypeStruct((order, width), jnp.bfloat16),
            in_specs=[pl.BlockSpec(memory_space=pltpu.VMEM)],
            out_specs=pl.BlockSpec(memory_space=pltpu.HBM),
            scratch_shapes=[
                pltpu.VMEM((order, width), jnp.bfloat16),
                pltpu.SemaphoreType.DMA((16,)),
            ],
            compiler_params=pltpu.CompilerParams(vmem_limit_bytes=16 * 2**20),
        )(acc)

    return jax.shard_map(local, mesh=mesh, in_specs=(P("batch", "col"), P("batch", "col")),
                         out_specs=P("batch", "col"), check_vma=False)
```

```python
import functools

import jax
import jax.numpy as jnp
from jax import lax
from jax.experimental import pallas as pl
from jax.experimental.pallas import tpu as pltpu
from jax.sharding import PartitionSpec as P

BLOCK = 256
MESH = pl.DeviceIdType.MESH
CHIPS = 8
PLUS_HOPS = (2, 2, 3, 5, 4, 4, 3, 2)
LONGER = {(0, 3): 12, (1, 3): 7, (1, 4): 13, (2, 4): 6, (2, 5): 8}
UP = 1
SLOTS = 36
RING = 19
LAPS = 8
LATER = (0, 3)


def pick(index, values):
    out = jnp.int32(values[-1])
    for j in range(len(values) - 2, -1, -1):
        out = jnp.where(index == j, jnp.int32(values[j]), out)
    return out


def kernel(nb, l_ref, b_ref, acc, lv, dg, raw, bv, isem, osem, fsem, dsem, bsem, credit):
    c = lax.axis_index("col")
    z, p = c // 2, c % 2
    q = 1 - p
    mate = z * 2 + q
    way = 1 - 2 * UP
    ahead = ((z + CHIPS + way * (1 - 2 * p)) % CHIPS) * 2 + p
    behind = ((z + CHIPS - way * (1 - 2 * p)) % CHIPS) * 2 + p
    half = BLOCK // 2
    first_slots = nb - 2 * z
    later = pick(p, LATER)

    def split(s, d, par):
        t = jnp.where(d <= pick(s, PLUS_HOPS), 0, nb)
        for (s0, d0), v in LONGER.items():
            t = jnp.where(s * CHIPS + d == s0 * CHIPS + d0, v, t)
        return t

    def source(core, d):
        return (z + CHIPS - way * (1 - 2 * core) * d) % CHIPS

    def bounds(core, d, par):
        s = source(core, d)
        k = 2 * s + par
        plus = core == UP
        here = split(s, jnp.where(plus, d, CHIPS - d), par)
        on = split(s, jnp.where(plus, d + 1, CHIPS - 1 - d), par)
        low = jnp.where(plus, jnp.maximum(k, here), k)
        high = jnp.where(plus, nb, here)
        on_low = jnp.where(plus, jnp.maximum(k, on), k)
        on_high = jnp.where(plus, nb, on)
        return k, low, high, on_low, on_high

    def inside(i, low, high):
        return (i >= low) & (i < high)

    def ends(core, d):
        _, l0, h0, _, _ = bounds(core, d, 0)
        _, l1, h1, _, _ = bounds(core, d, 1)
        return jnp.minimum(l0, l1), jnp.maximum(h0, h1)

    def start(core, d):
        low, high = ends(core, d)
        return jnp.where(low < high, jnp.where(core == UP, high - 1, low), -1)

    def advance(core, d, i):
        low, high = ends(core, d)
        j = jnp.where(core == UP, i - 1, i + 1)
        more = inside(j, low, high)
        ended = i < 0
        j = jnp.where(more, j, start(core, d + 1))
        return jnp.where(more | ended, d, d + 1), jnp.where(ended, i, j)

    def tiles(core, d, i):
        out = []
        for par in range(2):
            k, low, high, on_low, on_high = bounds(core, d, par)
            out.append((k, inside(i, low, high), inside(i, on_low, on_high)))
        return out

    def slot(k, i):
        return nb * k - k * (k - 1) // 2 + i - k

    def each(k, i, fn):
        @pl.when(i == k)
        def _():
            fn(dg.at[k])

        @pl.when(i != k)
        def _():
            fn(lv.at[slot(k, i)])

    def remote(ref, out, arrive, dev):
        return pltpu.make_async_remote_copy(
            src_ref=ref, dst_ref=ref, send_sem=out, recv_sem=arrive,
            device_id={"col": dev}, device_id_type=MESH)

    def send(k, i, out, arrive, dev):
        each(k, i, lambda ref: remote(ref, out, arrive, dev).start())

    def sent(k, i, out, dev):
        each(k, i, lambda ref: remote(ref, out, isem.at[0], dev).wait_send())

    def land(k, i, arrive):
        each(k, i, lambda ref: remote(ref, fsem.at[0], arrive, ahead).wait_recv())

    def out_sem(m, par):
        return fsem.at[(m % RING) * 2 + par]

    barrier = pltpu.get_barrier_semaphore()
    for dev in (behind, mate):
        pl.semaphore_signal(barrier, inc=1, device_id={"col": dev}, device_id_type=MESH)

    diag_row = pl.multiple_of(c * BLOCK, BLOCK)
    quarter = [
        pltpu.make_async_copy(l_ref.at[pl.ds(diag_row, half), pl.ds(0, half)], raw.at[0], fsem.at[0]),
        pltpu.make_async_copy(l_ref.at[pl.ds(diag_row + half, half), pl.ds(half, half)], raw.at[1], fsem.at[1]),
        pltpu.make_async_copy(
            l_ref.at[pl.ds(diag_row + half, half), pl.ds(0, half)], dg.at[c, pl.ds(half, half), :], fsem.at[2]),
    ]
    for copy in quarter:
        copy.start()
    row = lax.broadcasted_iota(jnp.int32, (half, half), 0)
    col = lax.broadcasted_iota(jnp.int32, (half, half), 1)

    def own_copy(i):
        rows = pl.ds(pl.multiple_of(i * BLOCK, BLOCK), BLOCK)
        return pltpu.make_async_copy(l_ref.at[rows, :], lv.at[slot(c, i)], dsem.at[i])

    def b_copy(k):
        rows = pl.ds(pl.multiple_of(k * BLOCK, BLOCK), BLOCK)
        return pltpu.make_async_copy(b_ref.at[rows, :], bv.at[rows, :], bsem)

    lax.fori_loop(c + 1, nb, lambda i, x: (own_copy(i).start(), x)[1], 0)
    for copy in quarter:
        copy.wait()
    corner = raw[1].astype(jnp.float32)
    dg[c, :half, :] = jnp.where(row >= col, raw[0].astype(jnp.float32), corner.T).astype(dg.dtype)
    line = jnp.sum(jnp.where(row == col, corner, 0.0), axis=0, keepdims=True)
    dg[c, BLOCK:, :] = jnp.broadcast_to(line, (dg.shape[1] - BLOCK, half)).astype(dg.dtype)
    lax.fori_loop(c + 1, nb, lambda i, x: (own_copy(i).wait(), x)[1], 0)
    lax.fori_loop(0, nb, lambda k, x: (b_copy(k).start(), x)[1], 0)
    with jax.named_scope('barr'):
        pl.semaphore_wait(barrier, 2)

    head = jnp.where(p == UP, 0, p)
    send(c, jnp.where(p == UP, nb - 1, c), out_sem(head, p), isem.at[head * 2 + p], ahead)
    def to_mate(j, carry):
        i = jnp.where(p == UP, c + j, nb - 1 - j)
        send(c, i, dsem.at[i], osem.at[i], mate)
        return carry

    lax.fori_loop(0, nb - c, to_mate, 0)

    def send_first(j, carry):
        i = jnp.where(p == UP, nb - 1 - j, 2 * z + j)

        @pl.when((i >= c) & (j != head))
        def _():
            send(c, i, out_sem(j, p), isem.at[j * 2 + p], ahead)

        @pl.when(i >= mate)
        def _():
            land(mate, i, osem.at[i])
            send(mate, i, out_sem(j, q), isem.at[j * 2 + q], ahead)

        return carry

    with jax.named_scope('first'):
        lax.fori_loop(0, first_slots, send_first, 0)

    pl.semaphore_signal(credit, inc=LAPS, device_id={"col": mate}, device_id_type=MESH)
    lax.fori_loop(c, nb, lambda i, x: (sent(c, i, dsem.at[i], mate), x)[1], 0)

    def clear(i, carry):
        acc[pl.ds(pl.multiple_of(i * 64, 64), 64), :] = jnp.zeros((64, acc.shape[1]), jnp.float32)
        return carry

    lax.fori_loop(0, acc.shape[0] // 64, clear, 0)
    with jax.named_scope('bwait'):
        pltpu.make_async_copy(b_ref, bv, bsem).wait()

    width = acc.shape[1] // 2

    def pair(k, i):
        at = pl.multiple_of(i * BLOCK, BLOCK)
        depth = pl.multiple_of(k * BLOCK, BLOCK)
        left, right = lv[slot(k, i)], lv[slot(k + 1, i)]
        for n in range(2):
            cols = slice(n * width, (n + 1) * width)
            acc[pl.ds(at, BLOCK), cols] += jnp.dot(
                left, bv[pl.ds(depth, BLOCK), cols], preferred_element_type=jnp.float32) + jnp.dot(
                right, bv[pl.ds(depth + BLOCK, BLOCK), cols], preferred_element_type=jnp.float32)

    def multiply(k, i):
        at = pl.multiple_of(i * BLOCK, BLOCK)
        depth = pl.multiple_of(k * BLOCK, BLOCK)

        @pl.when(i != k)
        def _():
            tile = lv[slot(k, i)]
            for n in range(2):
                cols = slice(n * width, (n + 1) * width)
                acc[pl.ds(at, BLOCK), cols] += jnp.dot(
                    tile, bv[pl.ds(depth, BLOCK), cols], preferred_element_type=jnp.float32)

        @pl.when(i == k)
        def _():
            both = dg[k, :half, :].astype(jnp.float32)
            line = dg[k, BLOCK:BLOCK + 1, :].astype(jnp.float32)
            top = jnp.where(row >= col, both, 0.0).astype(lv.dtype)
            left = dg[k, half:BLOCK, :]
            corner = jnp.where(row < col, both, jnp.where(row == col, line, 0.0)).T.astype(lv.dtype)
            for n in range(2):
                cols = slice(n * width, (n + 1) * width)
                upper = bv[pl.ds(depth, half), cols]
                lower = bv[pl.ds(depth + half, half), cols]
                acc[pl.ds(at, half), cols] += jnp.dot(top, upper, preferred_element_type=jnp.float32)
                acc[pl.ds(at + half, half), cols] += jnp.dot(
                    left, upper, preferred_element_type=jnp.float32) + jnp.dot(
                    corner, lower, preferred_element_type=jnp.float32)

    def left_onward(m, d, i):
        for par, (k, _, on) in enumerate(tiles(p, d, i)):
            @pl.when(on)
            def _():
                sent(k, i, out_sem(m, par), ahead)

        return advance(p, d, i)

    def use(k, r, v0, v1, from_mate, lap):
        for par, v in enumerate((v0, v1)):
            @pl.when(v & from_mate)
            def _():
                with jax.named_scope('mland'):
                    land(k + par, r, osem.at[lap + par])

        double = v0 & v1 & (r > k + 1)

        @pl.when(double)
        def _():
            pair(k, r)

        @pl.when(jnp.logical_not(double))
        def _():
            def single(par, carry):
                @pl.when(jnp.where(par == 0, v0.astype(jnp.int32), v1.astype(jnp.int32)) > 0)
                def _():
                    multiply(k + par, r)

                return carry

            lax.fori_loop(0, 2, single, 0)

    def step(n, cur):
        d, i, qd, qi, od, oi, gone = cur
        mine = tiles(p, d, i)
        lap = (n % LAPS) * 2

        pl.semaphore_wait(credit, 1)

        for par, (k, here, on) in enumerate(mine):
            @pl.when(here)
            def _():
                with jax.named_scope('land'):
                    land(k, i, isem.at[n * 2 + par])

                @pl.when(on)
                def _():
                    send(k, i, out_sem(first_slots + n, par), isem.at[gone * 2 + par], ahead)

                send(k, i, dsem.at[par], osem.at[lap + par], mate)

        late = n >= later
        theirs = tiles(q, qd, jnp.where(late, qi, -1))
        at_home = 2 * z + n
        home = [(2 * z + par, (at_home >= 2 * z + par) & (at_home < nb)) for par in range(2)]
        groups = (
            (mine[0][0], i, mine[0][1], mine[1][1]),
            (home[0][0], at_home, home[0][1], home[1][1]),
            (theirs[0][0], qi, theirs[0][1], theirs[1][1]),
        )
        lap_in = ((n + LAPS - later) % LAPS) * 2

        def one(j, carry):
            k, r, v0, v1 = (
                jnp.where(j == 0, x, jnp.where(j == 1, y, w))
                for x, y, w in zip(*[(g[0], g[1], g[2].astype(jnp.int32), g[3].astype(jnp.int32)) for g in groups]))
            use(k, r, v0 > 0, v1 > 0, j == 2, lap_in)
            return carry

        with jax.named_scope('work'):
            lax.fori_loop(0, 3, one, 0)

        @pl.when(late & (n - later < SLOTS - LAPS))
        def _():
            pl.semaphore_signal(credit, inc=1, device_id={"col": mate}, device_id_type=MESH)

        for par, (k, here, _) in enumerate(mine):
            @pl.when(here)
            def _():
                sent(k, i, dsem.at[par], mate)

        again = n >= 2
        e, f = left_onward(jnp.maximum(n - 2, 0), od, jnp.where(again, oi, -1))
        gone = gone + (mine[0][2] | mine[1][2]).astype(jnp.int32)
        g, h = advance(q, qd, qi)
        return (*advance(p, d, i), jnp.where(late, g, qd), jnp.where(late, h, qi), jnp.where(again, e, od), jnp.where(again, f, oi), gone)

    zero, one_ = jnp.int32(0), jnp.int32(1)
    state = lax.fori_loop(0, SLOTS, step, (
        one_, start(p, one_), one_, start(q, one_), zero, start(p, zero), first_slots))
    qd, qi, od, oi = state[2:6]
    left = zero
    for ahead_d in range(2):
        for par in range(2):
            _, _, _, on_low, on_high = bounds(p, od + ahead_d, par)
            left = jnp.where((oi >= 0) & (on_low < on_high), first_slots + 2, left)
    with jax.named_scope('tail'):
        lax.fori_loop(0, left, lambda m, cur: left_onward(SLOTS - 2 + m, *cur), (od, oi))

    def drain(m, cur):
        qd, qi = cur
        (k, v0, _), (_, v1, _) = tiles(q, qd, qi)
        use(k, qi, v0, v1, m >= 0, (m % LAPS) * 2)
        return advance(q, qd, qi)

    with jax.named_scope('drain'):
        lax.fori_loop(SLOTS - later, SLOTS, drain, (qd, qi))


def round_kernel(x_ref, o_ref, buf, sem):
    n = sem.shape[0]
    rows = x_ref.shape[0] // n
    step = 64

    def copy(j):
        part = pl.ds(pl.multiple_of(j * rows, rows), rows)
        return pltpu.make_async_copy(buf.at[part, :], o_ref.at[part, :], sem.at[j])

    def one(j, carry):
        def some(m, carry):
            part = pl.ds(pl.multiple_of(j * rows + m * step, step), step)
            buf[part, :] = x_ref[part, :].astype(buf.dtype)
            return carry

        lax.fori_loop(0, rows // step, some, 0)
        copy(j).start()
        return carry

    lax.fori_loop(0, n, one, 0)
    lax.fori_loop(0, n, lambda j, x: (copy(j).wait(), x)[1], 0)


def solution(mesh):
    def local(l_cols, b_cols):
        order, width = b_cols.shape
        nb = order // BLOCK
        tiles = nb * (nb + 1) // 2
        l_cols = pltpu.with_memory_space_constraint(l_cols, pltpu.HBM)
        b_cols = pltpu.with_memory_space_constraint(b_cols, pltpu.HBM)
        acc = pl.pallas_call(
            functools.partial(kernel, nb),
            out_shape=pltpu.VMEM((order, width), jnp.float32),
            in_specs=[pl.BlockSpec(memory_space=pltpu.HBM)] * 2,
            out_specs=pl.BlockSpec(memory_space=pltpu.VMEM),
            scratch_shapes=[
                pltpu.VMEM((tiles, BLOCK, BLOCK), jnp.bfloat16),
                pltpu.VMEM((nb, BLOCK + 16, BLOCK // 2), jnp.bfloat16),
                pltpu.VMEM((2, BLOCK // 2, BLOCK // 2), jnp.bfloat16),
                pltpu.VMEM((order, width), jnp.bfloat16),
                pltpu.SemaphoreType.DMA((2 * SLOTS,)),
                pltpu.SemaphoreType.DMA((max(nb, 2 * LAPS),)),
                pltpu.SemaphoreType.DMA((2 * RING,)),
                pltpu.SemaphoreType.DMA((nb,)),
                pltpu.SemaphoreType.DMA,
                pltpu.SemaphoreType.REGULAR,
            ],
            compiler_params=pltpu.CompilerParams(
                collective_id=0, has_side_effects=True, vmem_limit_bytes=34 * 2**20),
        )(l_cols, b_cols)
        return pl.pallas_call(
            round_kernel,
            out_shape=jax.ShapeDtypeStruct((order, width), jnp.bfloat16),
            in_specs=[pl.BlockSpec(memory_space=pltpu.VMEM)],
            out_specs=pl.BlockSpec(memory_space=pltpu.HBM),
            scratch_shapes=[
                pltpu.VMEM((order, width), jnp.bfloat16),
                pltpu.SemaphoreType.DMA((16,)),
            ],
            compiler_params=pltpu.CompilerParams(vmem_limit_bytes=16 * 2**20),
        )(acc)

    return jax.shard_map(local, mesh=mesh, in_specs=(P("batch", "col"), P("batch", "col")),
                         out_specs=P("batch", "col"), check_vma=False)
```

```python
import functools

import jax
import jax.numpy as jnp
from jax import lax
from jax.experimental import pallas as pl
from jax.experimental.pallas import tpu as pltpu
from jax.sharding import PartitionSpec as P

BLOCK = 256
MESH = pl.DeviceIdType.MESH
CHIPS = 8
PLUS_HOPS = (2, 2, 3, 5, 4, 4, 3, 2)
LONGER = {(0, 3): 12, (1, 3): 7, (1, 4): 13, (2, 4): 6, (2, 5): 8}
UP = 1
SPARE = 16
SLOTS = 36
RING = 19
LAPS = 8
LATER = (0, 3)


def pick(index, values):
    out = jnp.int32(values[-1])
    for j in range(len(values) - 2, -1, -1):
        out = jnp.where(index == j, jnp.int32(values[j]), out)
    return out


def kernel(nb, l_ref, b_ref, acc, lv, dg, raw, bv, isem, osem, fsem, dsem, bsem, credit):
    c = lax.axis_index("col")
    z, p = c // 2, c % 2
    q = 1 - p
    mate = z * 2 + q
    way = 1 - 2 * UP
    ahead = ((z + CHIPS + way * (1 - 2 * p)) % CHIPS) * 2 + p
    behind = ((z + CHIPS - way * (1 - 2 * p)) % CHIPS) * 2 + p
    half = BLOCK // 2
    first_slots = nb - 2 * z
    later = pick(p, LATER)

    def split(s, d):
        t = jnp.where(d <= pick(s, PLUS_HOPS), 0, nb)
        for (s0, d0), v in LONGER.items():
            t = jnp.where(s * CHIPS + d == s0 * CHIPS + d0, v, t)
        return t

    def bounds(core, d):
        s = (z + CHIPS - way * (1 - 2 * core) * d) % CHIPS
        plus = core == UP
        here = split(s, jnp.where(plus, d, CHIPS - d))
        on = split(s, jnp.where(plus, d + 1, CHIPS - 1 - d))
        low = jnp.where(plus, jnp.maximum(2 * s, here), 2 * s)
        high = jnp.where(plus, nb, here)
        on_low = jnp.where(plus, jnp.maximum(2 * s, on), 2 * s)
        on_high = jnp.where(plus, nb, on)
        return s, low, high, on_low, on_high

    def inside(i, low, high):
        return (i >= low) & (i < high)

    def start(core, d):
        _, low, high, _, _ = bounds(core, d)
        return jnp.where(low < high, jnp.where(core == UP, high - 1, low), -1)

    def advance(core, d, i):
        _, low, high, _, _ = bounds(core, d)
        j = jnp.where(core == UP, i - 1, i + 1)
        more = inside(j, low, high)
        ended = i < 0
        j = jnp.where(more, j, start(core, d + 1))
        return jnp.where(more | ended, d, d + 1), jnp.where(ended, i, j)

    def look(core, d, i):
        s, low, high, on_low, on_high = bounds(core, d)
        return s, inside(i, low, high), inside(i, on_low, on_high)

    def place(s, i):
        return (nb - 1) * s - s * (s - 1) + i - 2 * s - 1

    def each(k, i, fn):
        @pl.when(i == k)
        def _():
            fn(dg.at[k])

        @pl.when(i != k)
        def _():
            fn(lv.at[place(k // 2, i), k % 2])

    def strip(s, i, fn, whole):
        @pl.when(i == 2 * s)
        def _():
            fn(dg.at[i])

        @pl.when(i == 2 * s + 1)
        def _():
            if whole:
                fn(bv.at[pl.ds(0, 3 * BLOCK + SPARE), pl.ds(0, half)])
            else:
                fn(lv.at[place(s, i), 0])
                fn(dg.at[i])

        @pl.when(i > 2 * s + 1)
        def _():
            fn(lv.at[place(s, i)])

    def remote(ref, out, arrive, dev):
        return pltpu.make_async_remote_copy(
            src_ref=ref, dst_ref=ref, send_sem=out, recv_sem=arrive,
            device_id={"col": dev}, device_id_type=MESH)

    def send(s, i, out, arrive, dev):
        strip(s, i, lambda ref: remote(ref, out, arrive, dev).start(), False)

    def sent(s, i, out, dev):
        strip(s, i, lambda ref: remote(ref, out, isem.at[0], dev).wait_send(), True)

    def land(s, i, arrive):
        strip(s, i, lambda ref: remote(ref, fsem.at[0], arrive, ahead).wait_recv(), True)

    def out_sem(m):
        return fsem.at[m % RING]

    barrier = pltpu.get_barrier_semaphore()
    for dev in (behind, mate):
        pl.semaphore_signal(barrier, inc=1, device_id={"col": dev}, device_id_type=MESH)

    diag_row = pl.multiple_of(c * BLOCK, BLOCK)
    quarter = [
        pltpu.make_async_copy(l_ref.at[pl.ds(diag_row, half), pl.ds(0, half)], raw.at[0], fsem.at[0]),
        pltpu.make_async_copy(l_ref.at[pl.ds(diag_row + half, half), pl.ds(half, half)], raw.at[1], fsem.at[1]),
        pltpu.make_async_copy(
            l_ref.at[pl.ds(diag_row + half, half), pl.ds(0, half)], dg.at[c, pl.ds(half, half), :], fsem.at[2]),
    ]
    for copy in quarter:
        copy.start()
    row = lax.broadcasted_iota(jnp.int32, (half, half), 0)
    col = lax.broadcasted_iota(jnp.int32, (half, half), 1)

    def own_copy(i):
        rows = pl.ds(pl.multiple_of(i * BLOCK, BLOCK), BLOCK)
        return pltpu.make_async_copy(l_ref.at[rows, :], lv.at[place(z, i), p], dsem.at[i])

    def b_copy(k):
        rows = pl.ds(pl.multiple_of(k * BLOCK, BLOCK), BLOCK)
        return pltpu.make_async_copy(b_ref.at[rows, :], bv.at[rows, :], bsem)

    lax.fori_loop(c + 1, nb, lambda i, x: (own_copy(i).start(), x)[1], 0)
    for copy in quarter:
        copy.wait()
    corner = raw[1].astype(jnp.float32)
    dg[c, :half, :] = jnp.where(row >= col, raw[0].astype(jnp.float32), corner.T).astype(dg.dtype)
    line = jnp.sum(jnp.where(row == col, corner, 0.0), axis=0, keepdims=True)
    dg[c, BLOCK:, :] = jnp.broadcast_to(line, (SPARE, half)).astype(dg.dtype)
    lax.fori_loop(c + 1, nb, lambda i, x: (own_copy(i).wait(), x)[1], 0)
    lax.fori_loop(0, nb, lambda k, x: (b_copy(k).start(), x)[1], 0)
    pl.semaphore_wait(barrier, 2)

    def send_tile(k, i, out, arrive, dev):
        each(k, i, lambda ref: remote(ref, out, arrive, dev).start())

    head = jnp.where(p == UP, 0, p)
    send_tile(c, jnp.where(p == UP, nb - 1, c), out_sem(head), isem.at[head], ahead)

    def to_mate(j, carry):
        i = jnp.where(p == UP, c + j, nb - 1 - j)
        send_tile(c, i, dsem.at[i], osem.at[i], mate)
        return carry

    lax.fori_loop(0, nb - c, to_mate, 0)

    def send_first(j, carry):
        i = jnp.where(p == UP, nb - 1 - j, 2 * z + j)

        @pl.when((i >= c) & (j != head))
        def _():
            send_tile(c, i, out_sem(j), isem.at[j], ahead)

        @pl.when(i >= mate)
        def _():
            each(mate, i, lambda ref: remote(ref, fsem.at[0], osem.at[i], ahead).wait_recv())
            send_tile(mate, i, out_sem(j), isem.at[j], ahead)

        return carry

    lax.fori_loop(0, first_slots, send_first, 0)
    pl.semaphore_signal(credit, inc=LAPS, device_id={"col": mate}, device_id_type=MESH)

    def mate_has(i, carry):
        each(c, i, lambda ref: remote(ref, dsem.at[i], isem.at[0], mate).wait_send())
        return carry

    lax.fori_loop(c, nb, mate_has, 0)

    def clear(i, carry):
        acc[pl.ds(pl.multiple_of(i * 64, 64), 64), :] = jnp.zeros((64, acc.shape[1]), jnp.float32)
        return carry

    lax.fori_loop(0, acc.shape[0] // 64, clear, 0)
    pltpu.make_async_copy(b_ref, bv, bsem).wait()

    width = acc.shape[1] // 2
    parts = [slice(n * width, (n + 1) * width) for n in range(2)]

    def use(s, i):
        at = pl.multiple_of(i * BLOCK, BLOCK)
        depth = pl.multiple_of(2 * s * BLOCK, BLOCK)

        @pl.when(i > 2 * s + 1)
        def _():
            left, right = lv[place(s, i), 0], lv[place(s, i), 1]
            for cols in parts:
                acc[pl.ds(at, BLOCK), cols] += jnp.dot(
                    left, bv[pl.ds(depth, BLOCK), cols], preferred_element_type=jnp.float32) + jnp.dot(
                    right, bv[pl.ds(depth + BLOCK, BLOCK), cols], preferred_element_type=jnp.float32)

        @pl.when(i == 2 * s + 1)
        def _():
            left = lv[place(s, i), 0]
            for cols in parts:
                acc[pl.ds(at, BLOCK), cols] += jnp.dot(
                    left, bv[pl.ds(depth, BLOCK), cols], preferred_element_type=jnp.float32)

        @pl.when(i <= 2 * s + 1)
        def _():
            both = dg[i, :half, :].astype(jnp.float32)
            line = dg[i, BLOCK:BLOCK + 1, :].astype(jnp.float32)
            top = jnp.where(row >= col, both, 0.0).astype(lv.dtype)
            left = dg[i, half:BLOCK, :]
            corner = jnp.where(row < col, both, jnp.where(row == col, line, 0.0)).T.astype(lv.dtype)
            for cols in parts:
                upper = bv[pl.ds(at, half), cols]
                lower = bv[pl.ds(at + half, half), cols]
                acc[pl.ds(at, half), cols] += jnp.dot(top, upper, preferred_element_type=jnp.float32)
                acc[pl.ds(at + half, half), cols] += jnp.dot(
                    left, upper, preferred_element_type=jnp.float32) + jnp.dot(
                    corner, lower, preferred_element_type=jnp.float32)

    def left_onward(m, d, i):
        s, _, on = look(p, d, i)

        @pl.when(on)
        def _():
            sent(s, i, out_sem(m), ahead)

        return advance(p, d, i)

    def step(n, cur):
        d, i, qd, qi, od, oi, gone = cur
        s, here, on = look(p, d, i)
        pl.semaphore_wait(credit, 1)

        @pl.when(here)
        def _():
            land(s, i, isem.at[n])

            @pl.when(on)
            def _():
                send(s, i, out_sem(first_slots + n), isem.at[gone], ahead)

            send(s, i, dsem.at[0], osem.at[n % LAPS], mate)

        late = n >= later
        qs, there, _ = look(q, qd, jnp.where(late, qi, -1))
        lap_in = (n + LAPS - later) % LAPS
        at_home = 2 * z + n
        groups = ((s, i, here), (z, at_home, at_home < nb), (qs, qi, there))

        def one(j, carry):
            k, r, v = (
                jnp.where(j == 0, x, jnp.where(j == 1, y, w))
                for x, y, w in zip(*[(g[0], g[1], g[2].astype(jnp.int32)) for g in groups]))

            @pl.when(v > 0)
            def _():
                @pl.when(j == 2)
                def _():
                    land(k, r, osem.at[lap_in])

                use(k, r)

            return carry

        lax.fori_loop(0, 3, one, 0)

        @pl.when(late & (n - later < SLOTS - LAPS))
        def _():
            pl.semaphore_signal(credit, inc=1, device_id={"col": mate}, device_id_type=MESH)

        @pl.when(here)
        def _():
            sent(s, i, dsem.at[0], mate)

        again = n >= 2
        e, f = left_onward(jnp.maximum(n - 2, 0), od, jnp.where(again, oi, -1))
        g, h = advance(q, qd, qi)
        return (*advance(p, d, i), jnp.where(late, g, qd), jnp.where(late, h, qi),
                jnp.where(again, e, od), jnp.where(again, f, oi), gone + on.astype(jnp.int32))

    zero, one_ = jnp.int32(0), jnp.int32(1)
    state = lax.fori_loop(0, SLOTS, step, (
        one_, start(p, one_), one_, start(q, one_), zero, start(p, zero), first_slots))
    qd, qi, od, oi = state[2:6]
    left = zero
    for more in range(2):
        _, _, _, on_low, on_high = bounds(p, od + more)
        left = jnp.where((oi >= 0) & (on_low < on_high), first_slots + 2, left)
    lax.fori_loop(0, left, lambda m, cur: left_onward(SLOTS - 2 + m, *cur), (od, oi))

    def drain(m, cur):
        qd, qi = cur
        s, there, _ = look(q, qd, qi)

        @pl.when(there)
        def _():
            land(s, qi, osem.at[m % LAPS])
            use(s, qi)

        return advance(q, qd, qi)

    lax.fori_loop(SLOTS - later, SLOTS, drain, (qd, qi))


def round_kernel(x_ref, o_ref, buf, sem):
    chunks, step = 16, 64
    rows = x_ref.shape[0] // chunks
    step = min(step, rows)

    def one(j, carry):
        def some(m, carry):
            part = pl.ds(pl.multiple_of(j * rows + m * step, step), step)
            buf[part, :] = x_ref[part, :].astype(buf.dtype)
            return carry

        lax.fori_loop(0, rows // step, some, 0)
        part = pl.ds(pl.multiple_of(j * rows, rows), rows)
        pltpu.make_async_copy(buf.at[part, :], o_ref.at[part, :], sem).start()
        return carry

    lax.fori_loop(0, chunks, one, 0)
    pltpu.make_async_copy(buf, o_ref, sem).wait()


def solution(mesh):
    def local(l_cols, b_cols):
        order, width = b_cols.shape
        nb = order // BLOCK
        strips = sum(nb - 1 - 2 * s for s in range(nb // 2))
        l_cols = pltpu.with_memory_space_constraint(l_cols, pltpu.HBM)
        b_cols = pltpu.with_memory_space_constraint(b_cols, pltpu.HBM)
        acc = pl.pallas_call(
            functools.partial(kernel, nb),
            out_shape=pltpu.VMEM((order, width), jnp.float32),
            in_specs=[pl.BlockSpec(memory_space=pltpu.HBM)] * 2,
            out_specs=pl.BlockSpec(memory_space=pltpu.VMEM),
            scratch_shapes=[
                pltpu.VMEM((strips, 2, BLOCK, BLOCK), jnp.bfloat16),
                pltpu.VMEM((nb, BLOCK + SPARE, BLOCK // 2), jnp.bfloat16),
                pltpu.VMEM((2, BLOCK // 2, BLOCK // 2), jnp.bfloat16),
                pltpu.VMEM((order, width), jnp.bfloat16),
                pltpu.SemaphoreType.DMA((SLOTS,)),
                pltpu.SemaphoreType.DMA((max(nb, LAPS),)),
                pltpu.SemaphoreType.DMA((RING,)),
                pltpu.SemaphoreType.DMA((nb,)),
                pltpu.SemaphoreType.DMA,
                pltpu.SemaphoreType.REGULAR,
            ],
            compiler_params=pltpu.CompilerParams(
                collective_id=0, has_side_effects=True, vmem_limit_bytes=34 * 2**20),
        )(l_cols, b_cols)
        return pl.pallas_call(
            round_kernel,
            out_shape=jax.ShapeDtypeStruct((order, width), jnp.bfloat16),
            in_specs=[pl.BlockSpec(memory_space=pltpu.VMEM)],
            out_specs=pl.BlockSpec(memory_space=pltpu.HBM),
            scratch_shapes=[
                pltpu.VMEM((order, width), jnp.bfloat16),
                pltpu.SemaphoreType.DMA,
            ],
            compiler_params=pltpu.CompilerParams(vmem_limit_bytes=16 * 2**20),
        )(acc)

    return jax.shard_map(local, mesh=mesh, in_specs=(P("batch", "col"), P("batch", "col")),
                         out_specs=P("batch", "col"), check_vma=False)
```

```python
import functools

import jax
import jax.numpy as jnp
from jax import lax
from jax.experimental import pallas as pl
from jax.experimental.pallas import tpu as pltpu
from jax.sharding import PartitionSpec as P

BLOCK = 256
MESH = pl.DeviceIdType.MESH
CHIPS = 8
PLUS_HOPS = (2, 2, 3, 5, 4, 4, 3, 2)
LONGER = {(0, 3): 12, (1, 3): 7, (1, 4): 13, (2, 4): 5, (2, 5): 7}
LATE_FIRST = (2, 7)
UP = 1
SPARE = 16
SLOTS = 37
RING = 19
LAPS = 8
LATER = (-1, 3)


def pick(index, values):
    out = jnp.int32(values[-1])
    for j in range(len(values) - 2, -1, -1):
        out = jnp.where(index == j, jnp.int32(values[j]), out)
    return out


def kernel(nb, l_ref, b_ref, acc, lv, dg, raw, bv, isem, osem, fsem, dsem, bsem, credit):
    c = lax.axis_index("col")
    z, p = c // 2, c % 2
    q = 1 - p
    mate = z * 2 + q
    way = 1 - 2 * UP
    ahead = ((z + CHIPS + way * (1 - 2 * p)) % CHIPS) * 2 + p
    behind = ((z + CHIPS - way * (1 - 2 * p)) % CHIPS) * 2 + p
    half = BLOCK // 2
    first_slots = nb - 2 * z
    later = pick(p, LATER)

    def split(s, d):
        t = jnp.where(d <= pick(s, PLUS_HOPS), 0, nb)
        for (s0, d0), v in LONGER.items():
            t = jnp.where(s * CHIPS + d == s0 * CHIPS + d0, v, t)
        return t

    def bounds(core, d):
        s = (z + CHIPS - way * (1 - 2 * core) * d) % CHIPS
        plus = core == UP
        here = split(s, jnp.where(plus, d, CHIPS - d))
        on = split(s, jnp.where(plus, d + 1, CHIPS - 1 - d))
        low = jnp.where(plus, jnp.maximum(2 * s, here), 2 * s)
        high = jnp.where(plus, nb, here)
        on_low = jnp.where(plus, jnp.maximum(2 * s, on), 2 * s)
        on_high = jnp.where(plus, nb, on)
        return s, low, high, on_low, on_high

    def inside(i, low, high):
        return (i >= low) & (i < high)

    def start(core, d):
        _, low, high, _, _ = bounds(core, d)
        return jnp.where(low < high, jnp.where(core == UP, high - 1, low), -1)

    def advance(core, d, i):
        _, low, high, _, _ = bounds(core, d)
        j = jnp.where(core == UP, i - 1, i + 1)
        more = inside(j, low, high)
        ended = i < 0
        j = jnp.where(more, j, start(core, d + 1))
        return jnp.where(more | ended, d, d + 1), jnp.where(ended, i, j)

    def strip_at(s, r):
        s0, last = LATE_FIRST
        moved = jnp.where(r < last, r + 1, 2 * s0)
        return jnp.where((s == s0) & inside(r, 2 * s0, last + 1), moved, r)

    def look(core, d, r):
        s, low, high, on_low, on_high = bounds(core, d)
        return s, strip_at(s, r), inside(r, low, high), inside(r, on_low, on_high)

    def place(s, i):
        return (nb - 1) * s - s * (s - 1) + i - 2 * s - 1

    def each(k, i, fn):
        @pl.when(i == k)
        def _():
            fn(dg.at[k])

        @pl.when(i != k)
        def _():
            fn(lv.at[place(k // 2, i), k % 2])

    def strip(s, i, fn, whole):
        @pl.when(i == 2 * s)
        def _():
            fn(dg.at[i])

        @pl.when(i == 2 * s + 1)
        def _():
            if whole:
                fn(bv.at[pl.ds(0, 3 * BLOCK + SPARE), pl.ds(0, half)])
            else:
                fn(lv.at[place(s, i), 0])
                fn(dg.at[i])

        @pl.when(i > 2 * s + 1)
        def _():
            fn(lv.at[place(s, i)])

    def remote(ref, out, arrive, dev):
        return pltpu.make_async_remote_copy(
            src_ref=ref, dst_ref=ref, send_sem=out, recv_sem=arrive,
            device_id={"col": dev}, device_id_type=MESH)

    def send(s, i, out, arrive, dev):
        strip(s, i, lambda ref: remote(ref, out, arrive, dev).start(), False)

    def sent(s, i, out, dev):
        strip(s, i, lambda ref: remote(ref, out, isem.at[0], dev).wait_send(), True)

    def land(s, i, arrive):
        strip(s, i, lambda ref: remote(ref, fsem.at[0], arrive, ahead).wait_recv(), True)

    def out_sem(m):
        return fsem.at[m % RING]

    barrier = pltpu.get_barrier_semaphore()
    for dev in (behind, mate):
        pl.semaphore_signal(barrier, inc=1, device_id={"col": dev}, device_id_type=MESH)

    diag_row = pl.multiple_of(c * BLOCK, BLOCK)
    quarter = [
        pltpu.make_async_copy(l_ref.at[pl.ds(diag_row, half), pl.ds(0, half)], raw.at[0], fsem.at[0]),
        pltpu.make_async_copy(l_ref.at[pl.ds(diag_row + half, half), pl.ds(half, half)], raw.at[1], fsem.at[1]),
        pltpu.make_async_copy(
            l_ref.at[pl.ds(diag_row + half, half), pl.ds(0, half)], dg.at[c, pl.ds(half, half), :], fsem.at[2]),
    ]
    for copy in quarter:
        copy.start()
    row = lax.broadcasted_iota(jnp.int32, (half, half), 0)
    col = lax.broadcasted_iota(jnp.int32, (half, half), 1)

    def own_copy(i):
        rows = pl.ds(pl.multiple_of(i * BLOCK, BLOCK), BLOCK)
        return pltpu.make_async_copy(l_ref.at[rows, :], lv.at[place(z, i), p], dsem.at[i])

    def b_copy(k):
        rows = pl.ds(pl.multiple_of(k * BLOCK, BLOCK), BLOCK)
        return pltpu.make_async_copy(b_ref.at[rows, :], bv.at[rows, :], bsem)

    lax.fori_loop(c + 1, nb, lambda i, x: (own_copy(i).start(), x)[1], 0)
    for copy in quarter:
        copy.wait()
    corner = raw[1].astype(jnp.float32)
    dg[c, :half, :] = jnp.where(row >= col, raw[0].astype(jnp.float32), corner.T).astype(dg.dtype)
    line = jnp.sum(jnp.where(row == col, corner, 0.0), axis=0, keepdims=True)
    dg[c, BLOCK:, :] = jnp.broadcast_to(line, (SPARE, half)).astype(dg.dtype)
    lax.fori_loop(c + 1, nb, lambda i, x: (own_copy(i).wait(), x)[1], 0)
    lax.fori_loop(0, nb, lambda k, x: (b_copy(k).start(), x)[1], 0)
    pl.semaphore_wait(barrier, 2)

    def send_tile(k, i, out, arrive, dev):
        each(k, i, lambda ref: remote(ref, out, arrive, dev).start())

    head = jnp.where(p == UP, 0, p)
    send_tile(c, jnp.where(p == UP, nb - 1, strip_at(z, 2 * z + head)), out_sem(head), isem.at[head], ahead)

    def to_mate(j, carry):
        i = jnp.where(p == UP, c + j, nb - 1 - j)
        send_tile(c, i, dsem.at[i], osem.at[i], mate)
        return carry

    lax.fori_loop(0, nb - c, to_mate, 0)

    def send_first(j, carry):
        i = strip_at(z, jnp.where(p == UP, nb - 1 - j, 2 * z + j))

        @pl.when((i >= c) & (j != head))
        def _():
            send_tile(c, i, out_sem(j), isem.at[j], ahead)

        @pl.when(i >= mate)
        def _():
            each(mate, i, lambda ref: remote(ref, fsem.at[0], osem.at[i], ahead).wait_recv())
            send_tile(mate, i, out_sem(j), isem.at[j], ahead)

        return carry

    lax.fori_loop(0, first_slots, send_first, 0)
    pl.semaphore_signal(credit, inc=LAPS, device_id={"col": mate}, device_id_type=MESH)

    def mate_has(i, carry):
        each(c, i, lambda ref: remote(ref, dsem.at[i], isem.at[0], mate).wait_send())
        return carry

    lax.fori_loop(c, nb, mate_has, 0)

    def clear(i, carry):
        acc[pl.ds(pl.multiple_of(i * 64, 64), 64), :] = jnp.zeros((64, acc.shape[1]), jnp.float32)
        return carry

    lax.fori_loop(0, acc.shape[0] // 64, clear, 0)
    pltpu.make_async_copy(b_ref, bv, bsem).wait()

    width = acc.shape[1] // 2
    parts = [slice(n * width, (n + 1) * width) for n in range(2)]

    def use(s, i):
        at = pl.multiple_of(i * BLOCK, BLOCK)
        depth = pl.multiple_of(2 * s * BLOCK, BLOCK)

        @pl.when(i > 2 * s + 1)
        def _():
            left, right = lv[place(s, i), 0], lv[place(s, i), 1]
            for cols in parts:
                acc[pl.ds(at, BLOCK), cols] += jnp.dot(
                    left, bv[pl.ds(depth, BLOCK), cols], preferred_element_type=jnp.float32) + jnp.dot(
                    right, bv[pl.ds(depth + BLOCK, BLOCK), cols], preferred_element_type=jnp.float32)

        @pl.when(i == 2 * s + 1)
        def _():
            left = lv[place(s, i), 0]
            for cols in parts:
                acc[pl.ds(at, BLOCK), cols] += jnp.dot(
                    left, bv[pl.ds(depth, BLOCK), cols], preferred_element_type=jnp.float32)

        @pl.when(i <= 2 * s + 1)
        def _():
            both = dg[i, :half, :].astype(jnp.float32)
            line = dg[i, BLOCK:BLOCK + 1, :].astype(jnp.float32)
            top = jnp.where(row >= col, both, 0.0).astype(lv.dtype)
            left = dg[i, half:BLOCK, :]
            corner = jnp.where(row < col, both, jnp.where(row == col, line, 0.0)).T.astype(lv.dtype)
            for cols in parts:
                upper = bv[pl.ds(at, half), cols]
                lower = bv[pl.ds(at + half, half), cols]
                acc[pl.ds(at, half), cols] += jnp.dot(top, upper, preferred_element_type=jnp.float32)
                acc[pl.ds(at + half, half), cols] += jnp.dot(
                    left, upper, preferred_element_type=jnp.float32) + jnp.dot(
                    corner, lower, preferred_element_type=jnp.float32)

    def left_onward(m, d, i):
        s, r, _, on = look(p, d, i)

        @pl.when(on)
        def _():
            sent(s, r, out_sem(m), ahead)

        return advance(p, d, i)

    def step(n, cur):
        d, i, qd, qi, od, oi, gone = cur
        s, r, here, on = look(p, d, i)
        pl.semaphore_wait(credit, 1)

        @pl.when(here)
        def _():
            land(s, r, isem.at[n])

            @pl.when(on)
            def _():
                send(s, r, out_sem(first_slots + n), isem.at[gone], ahead)

            send(s, r, dsem.at[0], osem.at[n % LAPS], mate)

        late = n >= later
        qs, qr, there, _ = look(q, qd, jnp.where(late, qi, -1))
        lap_in = (n + LAPS - later) % LAPS
        at_home = 2 * z + n
        groups = ((s, r, here), (z, at_home, at_home < nb), (qs, qr, there))

        def one(j, carry):
            k, h, v = (
                jnp.where(j == 0, x, jnp.where(j == 1, y, w))
                for x, y, w in zip(*[(g[0], g[1], g[2].astype(jnp.int32)) for g in groups]))

            @pl.when(v > 0)
            def _():
                @pl.when(j == 2)
                def _():
                    land(k, h, osem.at[lap_in])

                use(k, h)

            return carry

        lax.fori_loop(0, 3, one, 0)

        @pl.when(late & (n - later < SLOTS - LAPS))
        def _():
            pl.semaphore_signal(credit, inc=1, device_id={"col": mate}, device_id_type=MESH)

        @pl.when(here)
        def _():
            sent(s, r, dsem.at[0], mate)

        again = n >= 2
        e, f = left_onward(jnp.maximum(n - 2, 0), od, jnp.where(again, oi, -1))
        g, e2 = advance(q, qd, qi)
        return (*advance(p, d, i), jnp.where(late, g, qd), jnp.where(late, e2, qi),
                jnp.where(again, e, od), jnp.where(again, f, oi), gone + on.astype(jnp.int32))

    def drain(m, cur):
        qd, qi = cur
        s, r, there, _ = look(q, qd, qi)

        @pl.when(there)
        def _():
            land(s, r, osem.at[m % LAPS])
            use(s, r)

        @pl.when(m < SLOTS - LAPS)
        def _():
            pl.semaphore_signal(credit, inc=1, device_id={"col": mate}, device_id_type=MESH)

        return advance(q, qd, qi)

    zero, one_ = jnp.int32(0), jnp.int32(1)
    qd, qi = lax.fori_loop(0, jnp.maximum(-later, 0), drain, (one_, start(q, one_)))
    state = lax.fori_loop(0, SLOTS, step, (
        one_, start(p, one_), qd, qi, zero, start(p, zero), first_slots))
    qd, qi, od, oi = state[2:6]
    left = zero
    for more in range(2):
        _, _, _, on_low, on_high = bounds(p, od + more)
        left = jnp.where((oi >= 0) & (on_low < on_high), first_slots + 2, left)
    lax.fori_loop(0, left, lambda m, cur: left_onward(SLOTS - 2 + m, *cur), (od, oi))

    lax.fori_loop(SLOTS - later, SLOTS, drain, (qd, qi))


def round_kernel(x_ref, o_ref, buf, sem):
    chunks, step = 16, 64
    rows = x_ref.shape[0] // chunks
    step = min(step, rows)

    def one(j, carry):
        def some(m, carry):
            part = pl.ds(pl.multiple_of(j * rows + m * step, step), step)
            buf[part, :] = x_ref[part, :].astype(buf.dtype)
            return carry

        lax.fori_loop(0, rows // step, some, 0)
        part = pl.ds(pl.multiple_of(j * rows, rows), rows)
        pltpu.make_async_copy(buf.at[part, :], o_ref.at[part, :], sem).start()
        return carry

    lax.fori_loop(0, chunks, one, 0)
    pltpu.make_async_copy(buf, o_ref, sem).wait()


def solution(mesh):
    def local(l_cols, b_cols):
        order, width = b_cols.shape
        nb = order // BLOCK
        strips = sum(nb - 1 - 2 * s for s in range(nb // 2))
        l_cols = pltpu.with_memory_space_constraint(l_cols, pltpu.HBM)
        b_cols = pltpu.with_memory_space_constraint(b_cols, pltpu.HBM)
        acc = pl.pallas_call(
            functools.partial(kernel, nb),
            out_shape=pltpu.VMEM((order, width), jnp.float32),
            in_specs=[pl.BlockSpec(memory_space=pltpu.HBM)] * 2,
            out_specs=pl.BlockSpec(memory_space=pltpu.VMEM),
            scratch_shapes=[
                pltpu.VMEM((strips, 2, BLOCK, BLOCK), jnp.bfloat16),
                pltpu.VMEM((nb, BLOCK + SPARE, BLOCK // 2), jnp.bfloat16),
                pltpu.VMEM((2, BLOCK // 2, BLOCK // 2), jnp.bfloat16),
                pltpu.VMEM((order, width), jnp.bfloat16),
                pltpu.SemaphoreType.DMA((SLOTS,)),
                pltpu.SemaphoreType.DMA((max(nb, LAPS),)),
                pltpu.SemaphoreType.DMA((RING,)),
                pltpu.SemaphoreType.DMA((nb,)),
                pltpu.SemaphoreType.DMA,
                pltpu.SemaphoreType.REGULAR,
            ],
            compiler_params=pltpu.CompilerParams(
                collective_id=0, has_side_effects=True, vmem_limit_bytes=34 * 2**20),
        )(l_cols, b_cols)
        return pl.pallas_call(
            round_kernel,
            out_shape=jax.ShapeDtypeStruct((order, width), jnp.bfloat16),
            in_specs=[pl.BlockSpec(memory_space=pltpu.VMEM)],
            out_specs=pl.BlockSpec(memory_space=pltpu.HBM),
            scratch_shapes=[
                pltpu.VMEM((order, width), jnp.bfloat16),
                pltpu.SemaphoreType.DMA,
            ],
            compiler_params=pltpu.CompilerParams(vmem_limit_bytes=16 * 2**20),
        )(acc)

    return jax.shard_map(local, mesh=mesh, in_specs=(P("batch", "col"), P("batch", "col")),
                         out_specs=P("batch", "col"), check_vma=False)
```

```python
import functools

import jax
import jax.numpy as jnp
from jax import lax
from jax.experimental import pallas as pl
from jax.experimental.pallas import tpu as pltpu
from jax.sharding import PartitionSpec as P

BLOCK = 256
MESH = pl.DeviceIdType.MESH
CHIPS = 8
PLUS_HOPS = (2, 2, 3, 5, 4, 4, 3, 2)
LONGER = {(0, 3): 12, (1, 3): 7, (1, 4): 13, (2, 4): 6, (2, 5): 7}
LATE_FIRST = (2, 7)
UP = 1
SPARE = 16
SLOTS = 37
RING = 19
LAPS = 8
LATER = (-1, 3)


def pick(index, values):
    out = jnp.int32(values[-1])
    for j in range(len(values) - 2, -1, -1):
        out = jnp.where(index == j, jnp.int32(values[j]), out)
    return out


def kernel(nb, l_ref, b_ref, acc, lv, dg, raw, bv, isem, osem, fsem, dsem, bsem, credit):
    c = lax.axis_index("col")
    z, p = c // 2, c % 2
    q = 1 - p
    mate = z * 2 + q
    way = 1 - 2 * UP
    ahead = ((z + CHIPS + way * (1 - 2 * p)) % CHIPS) * 2 + p
    behind = ((z + CHIPS - way * (1 - 2 * p)) % CHIPS) * 2 + p
    half = BLOCK // 2
    first_slots = nb - 2 * z
    later = pick(p, LATER)

    def split(s, d):
        t = jnp.where(d <= pick(s, PLUS_HOPS), 0, nb)
        for (s0, d0), v in LONGER.items():
            t = jnp.where(s * CHIPS + d == s0 * CHIPS + d0, v, t)
        return t

    def bounds(core, d):
        s = (z + CHIPS - way * (1 - 2 * core) * d) % CHIPS
        plus = core == UP
        here = split(s, jnp.where(plus, d, CHIPS - d))
        on = split(s, jnp.where(plus, d + 1, CHIPS - 1 - d))
        low = jnp.where(plus, jnp.maximum(2 * s, here), 2 * s)
        high = jnp.where(plus, nb, here)
        on_low = jnp.where(plus, jnp.maximum(2 * s, on), 2 * s)
        on_high = jnp.where(plus, nb, on)
        return s, low, high, on_low, on_high

    def inside(i, low, high):
        return (i >= low) & (i < high)

    def start(core, d):
        _, low, high, _, _ = bounds(core, d)
        return jnp.where(low < high, jnp.where(core == UP, high - 1, low), -1)

    def advance(core, d, i):
        _, low, high, _, _ = bounds(core, d)
        j = jnp.where(core == UP, i - 1, i + 1)
        more = inside(j, low, high)
        ended = i < 0
        j = jnp.where(more, j, start(core, d + 1))
        return jnp.where(more | ended, d, d + 1), jnp.where(ended, i, j)

    def strip_at(s, r):
        s0, last = LATE_FIRST
        moved = jnp.where(r < last, r + 1, 2 * s0)
        return jnp.where((s == s0) & inside(r, 2 * s0, last + 1), moved, r)

    def look(core, d, r):
        s, low, high, on_low, on_high = bounds(core, d)
        return s, strip_at(s, r), inside(r, low, high), inside(r, on_low, on_high)

    def place(s, i):
        return (nb - 1) * s - s * (s - 1) + i - 2 * s - 1

    def each(k, i, fn):
        @pl.when(i == k)
        def _():
            fn(dg.at[k])

        @pl.when(i != k)
        def _():
            fn(lv.at[place(k // 2, i), k % 2])

    def strip(s, i, fn, whole):
        @pl.when(i == 2 * s)
        def _():
            fn(dg.at[i])

        @pl.when(i == 2 * s + 1)
        def _():
            if whole:
                fn(bv.at[pl.ds(0, 3 * BLOCK + SPARE), pl.ds(0, half)])
            else:
                fn(lv.at[place(s, i), 0])
                fn(dg.at[i])

        @pl.when(i > 2 * s + 1)
        def _():
            fn(lv.at[place(s, i)])

    def remote(ref, out, arrive, dev):
        return pltpu.make_async_remote_copy(
            src_ref=ref, dst_ref=ref, send_sem=out, recv_sem=arrive,
            device_id={"col": dev}, device_id_type=MESH)

    def send(s, i, out, arrive, dev):
        strip(s, i, lambda ref: remote(ref, out, arrive, dev).start(), False)

    def sent(s, i, out, dev):
        strip(s, i, lambda ref: remote(ref, out, isem.at[0], dev).wait_send(), True)

    def land(s, i, arrive):
        strip(s, i, lambda ref: remote(ref, fsem.at[0], arrive, ahead).wait_recv(), True)

    def out_sem(m):
        return fsem.at[m % RING]

    barrier = pltpu.get_barrier_semaphore()
    for dev in (behind, mate):
        pl.semaphore_signal(barrier, inc=1, device_id={"col": dev}, device_id_type=MESH)

    diag_row = pl.multiple_of(c * BLOCK, BLOCK)
    quarter = [
        pltpu.make_async_copy(l_ref.at[pl.ds(diag_row, half), pl.ds(0, half)], raw.at[0], fsem.at[0]),
        pltpu.make_async_copy(l_ref.at[pl.ds(diag_row + half, half), pl.ds(half, half)], raw.at[1], fsem.at[1]),
        pltpu.make_async_copy(
            l_ref.at[pl.ds(diag_row + half, half), pl.ds(0, half)], dg.at[c, pl.ds(half, half), :], fsem.at[2]),
    ]
    for copy in quarter:
        copy.start()
    row = lax.broadcasted_iota(jnp.int32, (half, half), 0)
    col = lax.broadcasted_iota(jnp.int32, (half, half), 1)

    def own_copy(i):
        rows = pl.ds(pl.multiple_of(i * BLOCK, BLOCK), BLOCK)
        return pltpu.make_async_copy(l_ref.at[rows, :], lv.at[place(z, i), p], dsem.at[i])

    def b_copy(k):
        rows = pl.ds(pl.multiple_of(k * BLOCK, BLOCK), BLOCK)
        return pltpu.make_async_copy(b_ref.at[rows, :], bv.at[rows, :], bsem)

    lax.fori_loop(c + 1, nb, lambda i, x: (own_copy(i).start(), x)[1], 0)
    for copy in quarter:
        copy.wait()
    corner = raw[1].astype(jnp.float32)
    dg[c, :half, :] = jnp.where(row >= col, raw[0].astype(jnp.float32), corner.T).astype(dg.dtype)
    line = jnp.sum(jnp.where(row == col, corner, 0.0), axis=0, keepdims=True)
    dg[c, BLOCK:, :] = jnp.broadcast_to(line, (SPARE, half)).astype(dg.dtype)
    lax.fori_loop(c + 1, nb, lambda i, x: (own_copy(i).wait(), x)[1], 0)
    lax.fori_loop(0, nb, lambda k, x: (b_copy(k).start(), x)[1], 0)
    pl.semaphore_wait(barrier, 2)

    def send_tile(k, i, out, arrive, dev):
        each(k, i, lambda ref: remote(ref, out, arrive, dev).start())

    head = jnp.where(p == UP, 0, p)
    send_tile(c, jnp.where(p == UP, nb - 1, strip_at(z, 2 * z + head)), out_sem(head), isem.at[head], ahead)

    def to_mate(j, carry):
        i = jnp.where(p == UP, c + j, nb - 1 - j)
        send_tile(c, i, dsem.at[i], osem.at[i], mate)
        return carry

    lax.fori_loop(0, nb - c, to_mate, 0)

    def send_first(j, carry):
        i = strip_at(z, jnp.where(p == UP, nb - 1 - j, 2 * z + j))

        @pl.when((i >= c) & (j != head))
        def _():
            send_tile(c, i, out_sem(j), isem.at[j], ahead)

        @pl.when(i >= mate)
        def _():
            each(mate, i, lambda ref: remote(ref, fsem.at[0], osem.at[i], ahead).wait_recv())
            send_tile(mate, i, out_sem(j), isem.at[j], ahead)

        return carry

    lax.fori_loop(0, first_slots, send_first, 0)
    pl.semaphore_signal(credit, inc=LAPS, device_id={"col": mate}, device_id_type=MESH)

    def mate_has(i, carry):
        each(c, i, lambda ref: remote(ref, dsem.at[i], isem.at[0], mate).wait_send())
        return carry

    lax.fori_loop(c, nb, mate_has, 0)

    def clear(i, carry):
        acc[pl.ds(pl.multiple_of(i * 64, 64), 64), :] = jnp.zeros((64, acc.shape[1]), jnp.float32)
        return carry

    lax.fori_loop(0, acc.shape[0] // 64, clear, 0)
    pltpu.make_async_copy(b_ref, bv, bsem).wait()

    width = acc.shape[1] // 2
    parts = [slice(n * width, (n + 1) * width) for n in range(2)]

    def use(s, i):
        at = pl.multiple_of(i * BLOCK, BLOCK)
        depth = pl.multiple_of(2 * s * BLOCK, BLOCK)

        @pl.when(i > 2 * s + 1)
        def _():
            left, right = lv[place(s, i), 0], lv[place(s, i), 1]
            for cols in parts:
                acc[pl.ds(at, BLOCK), cols] += jnp.dot(
                    left, bv[pl.ds(depth, BLOCK), cols], preferred_element_type=jnp.float32) + jnp.dot(
                    right, bv[pl.ds(depth + BLOCK, BLOCK), cols], preferred_element_type=jnp.float32)

        @pl.when(i == 2 * s + 1)
        def _():
            left = lv[place(s, i), 0]
            for cols in parts:
                acc[pl.ds(at, BLOCK), cols] += jnp.dot(
                    left, bv[pl.ds(depth, BLOCK), cols], preferred_element_type=jnp.float32)

        @pl.when(i <= 2 * s + 1)
        def _():
            both = dg[i, :half, :].astype(jnp.float32)
            line = dg[i, BLOCK:BLOCK + 1, :].astype(jnp.float32)
            top = jnp.where(row >= col, both, 0.0).astype(lv.dtype)
            left = dg[i, half:BLOCK, :]
            corner = jnp.where(row < col, both, jnp.where(row == col, line, 0.0)).T.astype(lv.dtype)
            for cols in parts:
                upper = bv[pl.ds(at, half), cols]
                lower = bv[pl.ds(at + half, half), cols]
                acc[pl.ds(at, half), cols] += jnp.dot(top, upper, preferred_element_type=jnp.float32)
                acc[pl.ds(at + half, half), cols] += jnp.dot(
                    left, upper, preferred_element_type=jnp.float32) + jnp.dot(
                    corner, lower, preferred_element_type=jnp.float32)

    def left_onward(m, d, i):
        s, r, _, on = look(p, d, i)

        @pl.when(on)
        def _():
            sent(s, r, out_sem(m), ahead)

        return advance(p, d, i)

    def step(n, cur):
        d, i, qd, qi, od, oi, gone = cur
        s, r, here, on = look(p, d, i)
        pl.semaphore_wait(credit, 1)

        @pl.when(here)
        def _():
            land(s, r, isem.at[n])

            @pl.when(on)
            def _():
                send(s, r, out_sem(first_slots + n), isem.at[gone], ahead)

            send(s, r, dsem.at[0], osem.at[n % LAPS], mate)

        late = n >= later
        qs, qr, there, _ = look(q, qd, jnp.where(late, qi, -1))
        lap_in = (n + LAPS - later) % LAPS
        at_home = 2 * z + n
        groups = ((s, r, here), (z, at_home, at_home < nb), (qs, qr, there))

        def one(j, carry):
            k, h, v = (
                jnp.where(j == 0, x, jnp.where(j == 1, y, w))
                for x, y, w in zip(*[(g[0], g[1], g[2].astype(jnp.int32)) for g in groups]))

            @pl.when(v > 0)
            def _():
                @pl.when(j == 2)
                def _():
                    land(k, h, osem.at[lap_in])

                use(k, h)

            return carry

        lax.fori_loop(0, 3, one, 0)

        @pl.when(late & (n - later < SLOTS - LAPS))
        def _():
            pl.semaphore_signal(credit, inc=1, device_id={"col": mate}, device_id_type=MESH)

        @pl.when(here)
        def _():
            sent(s, r, dsem.at[0], mate)

        again = n >= 2
        e, f = left_onward(jnp.maximum(n - 2, 0), od, jnp.where(again, oi, -1))
        g, e2 = advance(q, qd, qi)
        return (*advance(p, d, i), jnp.where(late, g, qd), jnp.where(late, e2, qi),
                jnp.where(again, e, od), jnp.where(again, f, oi), gone + on.astype(jnp.int32))

    def drain(m, cur):
        qd, qi = cur
        s, r, there, _ = look(q, qd, qi)

        @pl.when(there)
        def _():
            land(s, r, osem.at[m % LAPS])
            use(s, r)

        @pl.when(m < SLOTS - LAPS)
        def _():
            pl.semaphore_signal(credit, inc=1, device_id={"col": mate}, device_id_type=MESH)

        return advance(q, qd, qi)

    zero, one_ = jnp.int32(0), jnp.int32(1)
    qd, qi = lax.fori_loop(0, jnp.maximum(-later, 0), drain, (one_, start(q, one_)))
    state = lax.fori_loop(0, SLOTS, step, (
        one_, start(p, one_), qd, qi, zero, start(p, zero), first_slots))
    qd, qi, od, oi = state[2:6]
    left = zero
    for more in range(2):
        _, _, _, on_low, on_high = bounds(p, od + more)
        left = jnp.where((oi >= 0) & (on_low < on_high), first_slots + 2, left)
    lax.fori_loop(0, left, lambda m, cur: left_onward(SLOTS - 2 + m, *cur), (od, oi))

    lax.fori_loop(SLOTS - later, SLOTS, drain, (qd, qi))


def round_kernel(x_ref, o_ref, buf, sem):
    chunks, step = 16, 64
    rows = x_ref.shape[0] // chunks
    step = min(step, rows)

    def one(j, carry):
        def some(m, carry):
            part = pl.ds(pl.multiple_of(j * rows + m * step, step), step)
            buf[part, :] = x_ref[part, :].astype(buf.dtype)
            return carry

        lax.fori_loop(0, rows // step, some, 0)
        part = pl.ds(pl.multiple_of(j * rows, rows), rows)
        pltpu.make_async_copy(buf.at[part, :], o_ref.at[part, :], sem).start()
        return carry

    lax.fori_loop(0, chunks, one, 0)
    pltpu.make_async_copy(buf, o_ref, sem).wait()


def solution(mesh):
    def local(l_cols, b_cols):
        order, width = b_cols.shape
        nb = order // BLOCK
        strips = sum(nb - 1 - 2 * s for s in range(nb // 2))
        l_cols = pltpu.with_memory_space_constraint(l_cols, pltpu.HBM)
        b_cols = pltpu.with_memory_space_constraint(b_cols, pltpu.HBM)
        acc = pl.pallas_call(
            functools.partial(kernel, nb),
            out_shape=pltpu.VMEM((order, width), jnp.float32),
            in_specs=[pl.BlockSpec(memory_space=pltpu.HBM)] * 2,
            out_specs=pl.BlockSpec(memory_space=pltpu.VMEM),
            scratch_shapes=[
                pltpu.VMEM((strips, 2, BLOCK, BLOCK), jnp.bfloat16),
                pltpu.VMEM((nb, BLOCK + SPARE, BLOCK // 2), jnp.bfloat16),
                pltpu.VMEM((2, BLOCK // 2, BLOCK // 2), jnp.bfloat16),
                pltpu.VMEM((order, width), jnp.bfloat16),
                pltpu.SemaphoreType.DMA((SLOTS,)),
                pltpu.SemaphoreType.DMA((max(nb, LAPS),)),
                pltpu.SemaphoreType.DMA((RING,)),
                pltpu.SemaphoreType.DMA((nb,)),
                pltpu.SemaphoreType.DMA,
                pltpu.SemaphoreType.REGULAR,
            ],
            compiler_params=pltpu.CompilerParams(
                collective_id=0, has_side_effects=True, vmem_limit_bytes=34 * 2**20),
        )(l_cols, b_cols)
        return pl.pallas_call(
            round_kernel,
            out_shape=jax.ShapeDtypeStruct((order, width), jnp.bfloat16),
            in_specs=[pl.BlockSpec(memory_space=pltpu.VMEM)],
            out_specs=pl.BlockSpec(memory_space=pltpu.HBM),
            scratch_shapes=[
                pltpu.VMEM((order, width), jnp.bfloat16),
                pltpu.SemaphoreType.DMA,
            ],
            compiler_params=pltpu.CompilerParams(vmem_limit_bytes=16 * 2**20),
        )(acc)

    return jax.shard_map(local, mesh=mesh, in_specs=(P("batch", "col"), P("batch", "col")),
                         out_specs=P("batch", "col"), check_vma=False)
```

```python
import functools

import jax
import jax.numpy as jnp
from jax import lax
from jax.experimental import pallas as pl
from jax.experimental.pallas import tpu as pltpu
from jax.sharding import PartitionSpec as P

BLOCK = 256
MESH = pl.DeviceIdType.MESH
PLUS_HOPS = (2, 2, 3, 5, 4, 4, 3, 2)
LONGER = {(0, 3): 12, (1, 3): 7, (1, 4): 13, (2, 4): 6, (2, 5): 8}
UP = 1
SPARE = 16
SLOTS = 36
RING = 19
LAPS = 8
LATER = (0, 3)


def pick(index, values):
    out = jnp.int32(values[-1])
    for j in range(len(values) - 2, -1, -1):
        out = jnp.where(index == j, jnp.int32(values[j]), out)
    return out


def kernel(nb, chips, l_ref, b_ref, acc, lv, dg, raw, bv, isem, osem, fsem, dsem, bsem, credit):
    c = lax.axis_index("col")
    z, p = c // 2, c % 2
    q = 1 - p
    mate = z * 2 + q
    way = 1 - 2 * UP
    ahead = ((z + chips + way * (1 - 2 * p)) % chips) * 2 + p
    behind = ((z + chips - way * (1 - 2 * p)) % chips) * 2 + p
    half = BLOCK // 2
    first_slots = nb - 2 * z
    later = pick(p, LATER)

    def split(s, d):
        t = jnp.where(d <= pick(s, PLUS_HOPS), 0, nb)
        for (s0, d0), v in LONGER.items():
            t = jnp.where(s * chips + d == s0 * chips + d0, v, t)
        return t

    def bounds(core, d):
        s = (z + chips - way * (1 - 2 * core) * d) % chips
        plus = core == UP
        here = split(s, jnp.where(plus, d, chips - d))
        on = split(s, jnp.where(plus, d + 1, chips - 1 - d))
        low = jnp.where(plus, jnp.maximum(2 * s, here), 2 * s)
        high = jnp.where(plus, nb, here)
        on_low = jnp.where(plus, jnp.maximum(2 * s, on), 2 * s)
        on_high = jnp.where(plus, nb, on)
        return s, low, high, on_low, on_high

    def inside(i, low, high):
        return (i >= low) & (i < high)

    def start(core, d):
        _, low, high, _, _ = bounds(core, d)
        return jnp.where(low < high, jnp.where(core == UP, high - 1, low), -1)

    def advance(core, d, i):
        _, low, high, _, _ = bounds(core, d)
        j = jnp.where(core == UP, i - 1, i + 1)
        more = inside(j, low, high)
        ended = i < 0
        j = jnp.where(more, j, start(core, d + 1))
        return jnp.where(more | ended, d, d + 1), jnp.where(ended, i, j)

    def look(core, d, i):
        s, low, high, on_low, on_high = bounds(core, d)
        return s, inside(i, low, high), inside(i, on_low, on_high)

    def place(s, i):
        return (nb - 1) * s - s * (s - 1) + i - 2 * s - 1

    def each(k, i, fn):
        @pl.when(i == k)
        def _():
            fn(dg.at[k])

        @pl.when(i != k)
        def _():
            fn(lv.at[place(k // 2, i), k % 2])

    def strip(s, i, fn, whole):
        @pl.when(i == 2 * s)
        def _():
            fn(dg.at[i])

        @pl.when(i == 2 * s + 1)
        def _():
            if whole:
                fn(bv.at[pl.ds(0, 3 * BLOCK + SPARE), pl.ds(0, half)])
            else:
                fn(lv.at[place(s, i), 0])
                fn(dg.at[i])

        @pl.when(i > 2 * s + 1)
        def _():
            fn(lv.at[place(s, i)])

    def remote(ref, out, arrive, dev):
        return pltpu.make_async_remote_copy(
            src_ref=ref, dst_ref=ref, send_sem=out, recv_sem=arrive,
            device_id={"col": dev}, device_id_type=MESH)

    def send(s, i, out, arrive, dev):
        strip(s, i, lambda ref: remote(ref, out, arrive, dev).start(), False)

    def sent(s, i, out, dev):
        strip(s, i, lambda ref: remote(ref, out, isem.at[0], dev).wait_send(), True)

    def land(s, i, arrive):
        strip(s, i, lambda ref: remote(ref, fsem.at[0], arrive, ahead).wait_recv(), True)

    def out_sem(m):
        return fsem.at[m % RING]

    barrier = pltpu.get_barrier_semaphore()
    for dev in (behind, mate):
        pl.semaphore_signal(barrier, inc=1, device_id={"col": dev}, device_id_type=MESH)

    diag_row = pl.multiple_of(c * BLOCK, BLOCK)
    quarter = [
        pltpu.make_async_copy(l_ref.at[pl.ds(diag_row, half), pl.ds(0, half)], raw.at[0], fsem.at[0]),
        pltpu.make_async_copy(l_ref.at[pl.ds(diag_row + half, half), pl.ds(half, half)], raw.at[1], fsem.at[1]),
        pltpu.make_async_copy(
            l_ref.at[pl.ds(diag_row + half, half), pl.ds(0, half)], dg.at[c, pl.ds(half, half), :], fsem.at[2]),
    ]
    for copy in quarter:
        copy.start()
    row = lax.broadcasted_iota(jnp.int32, (half, half), 0)
    col = lax.broadcasted_iota(jnp.int32, (half, half), 1)

    def own_copy(i):
        rows = pl.ds(pl.multiple_of(i * BLOCK, BLOCK), BLOCK)
        return pltpu.make_async_copy(l_ref.at[rows, :], lv.at[place(z, i), p], dsem.at[i])

    def b_copy(k):
        rows = pl.ds(pl.multiple_of(k * BLOCK, BLOCK), BLOCK)
        return pltpu.make_async_copy(b_ref.at[rows, :], bv.at[rows, :], bsem)

    lax.fori_loop(c + 1, nb, lambda i, x: (own_copy(i).start(), x)[1], 0)
    for copy in quarter:
        copy.wait()
    corner = raw[1].astype(jnp.float32)
    dg[c, :half, :] = jnp.where(row >= col, raw[0].astype(jnp.float32), corner.T).astype(dg.dtype)
    line = jnp.sum(jnp.where(row == col, corner, 0.0), axis=0, keepdims=True)
    dg[c, BLOCK:, :] = jnp.broadcast_to(line, (SPARE, half)).astype(dg.dtype)
    lax.fori_loop(c + 1, nb, lambda i, x: (own_copy(i).wait(), x)[1], 0)
    lax.fori_loop(0, nb, lambda k, x: (b_copy(k).start(), x)[1], 0)
    pl.semaphore_wait(barrier, 2)

    def send_tile(k, i, out, arrive, dev):
        each(k, i, lambda ref: remote(ref, out, arrive, dev).start())

    head = jnp.where(p == UP, 0, p)
    send_tile(c, jnp.where(p == UP, nb - 1, c), out_sem(head), isem.at[head], ahead)

    def to_mate(j, carry):
        i = jnp.where(p == UP, c + j, nb - 1 - j)
        send_tile(c, i, dsem.at[i], osem.at[i], mate)
        return carry

    lax.fori_loop(0, nb - c, to_mate, 0)

    def send_first(j, carry):
        i = jnp.where(p == UP, nb - 1 - j, 2 * z + j)

        @pl.when((i >= c) & (j != head))
        def _():
            send_tile(c, i, out_sem(j), isem.at[j], ahead)

        @pl.when(i >= mate)
        def _():
            each(mate, i, lambda ref: remote(ref, fsem.at[0], osem.at[i], ahead).wait_recv())
            send_tile(mate, i, out_sem(j), isem.at[j], ahead)

        return carry

    lax.fori_loop(0, first_slots, send_first, 0)
    pl.semaphore_signal(credit, inc=LAPS, device_id={"col": mate}, device_id_type=MESH)

    def mate_has(i, carry):
        each(c, i, lambda ref: remote(ref, dsem.at[i], isem.at[0], mate).wait_send())
        return carry

    lax.fori_loop(c, nb, mate_has, 0)

    def clear(i, carry):
        acc[pl.ds(pl.multiple_of(i * 64, 64), 64), :] = jnp.zeros((64, acc.shape[1]), jnp.float32)
        return carry

    lax.fori_loop(0, acc.shape[0] // 64, clear, 0)
    pltpu.make_async_copy(b_ref, bv, bsem).wait()

    width = acc.shape[1] // 2
    parts = [slice(n * width, (n + 1) * width) for n in range(2)]

    def use(s, i):
        at = pl.multiple_of(i * BLOCK, BLOCK)
        depth = pl.multiple_of(2 * s * BLOCK, BLOCK)

        @pl.when(i > 2 * s + 1)
        def _():
            left, right = lv[place(s, i), 0], lv[place(s, i), 1]
            for cols in parts:
                acc[pl.ds(at, BLOCK), cols] += jnp.dot(
                    left, bv[pl.ds(depth, BLOCK), cols], preferred_element_type=jnp.float32) + jnp.dot(
                    right, bv[pl.ds(depth + BLOCK, BLOCK), cols], preferred_element_type=jnp.float32)

        @pl.when(i == 2 * s + 1)
        def _():
            left = lv[place(s, i), 0]
            for cols in parts:
                acc[pl.ds(at, BLOCK), cols] += jnp.dot(
                    left, bv[pl.ds(depth, BLOCK), cols], preferred_element_type=jnp.float32)

        @pl.when(i <= 2 * s + 1)
        def _():
            both = dg[i, :half, :].astype(jnp.float32)
            line = dg[i, BLOCK:BLOCK + 1, :].astype(jnp.float32)
            top = jnp.where(row >= col, both, 0.0).astype(lv.dtype)
            left = dg[i, half:BLOCK, :]
            corner = jnp.where(row < col, both, jnp.where(row == col, line, 0.0)).T.astype(lv.dtype)
            for cols in parts:
                upper = bv[pl.ds(at, half), cols]
                lower = bv[pl.ds(at + half, half), cols]
                acc[pl.ds(at, half), cols] += jnp.dot(top, upper, preferred_element_type=jnp.float32)
                acc[pl.ds(at + half, half), cols] += jnp.dot(
                    left, upper, preferred_element_type=jnp.float32) + jnp.dot(
                    corner, lower, preferred_element_type=jnp.float32)

    def left_onward(m, d, i):
        s, _, on = look(p, d, i)

        @pl.when(on)
        def _():
            sent(s, i, out_sem(m), ahead)

        return advance(p, d, i)

    def step(n, cur):
        d, i, qd, qi, od, oi, gone = cur
        s, here, on = look(p, d, i)
        pl.semaphore_wait(credit, 1)

        @pl.when(here)
        def _():
            land(s, i, isem.at[n])

            @pl.when(on)
            def _():
                send(s, i, out_sem(first_slots + n), isem.at[gone], ahead)

            send(s, i, dsem.at[0], osem.at[n % LAPS], mate)

        late = n >= later
        qs, there, _ = look(q, qd, jnp.where(late, qi, -1))
        lap_in = (n + LAPS - later) % LAPS
        at_home = 2 * z + n
        groups = ((s, i, here), (z, at_home, at_home < nb), (qs, qi, there))

        def one(j, carry):
            k, r, v = (
                jnp.where(j == 0, x, jnp.where(j == 1, y, w))
                for x, y, w in zip(*[(g[0], g[1], g[2].astype(jnp.int32)) for g in groups]))

            @pl.when(v > 0)
            def _():
                @pl.when(j == 2)
                def _():
                    land(k, r, osem.at[lap_in])

                use(k, r)

            return carry

        lax.fori_loop(0, 3, one, 0)

        @pl.when(late & (n - later < SLOTS - LAPS))
        def _():
            pl.semaphore_signal(credit, inc=1, device_id={"col": mate}, device_id_type=MESH)

        @pl.when(here)
        def _():
            sent(s, i, dsem.at[0], mate)

        again = n >= 2
        e, f = left_onward(jnp.maximum(n - 2, 0), od, jnp.where(again, oi, -1))
        g, h = advance(q, qd, qi)
        return (*advance(p, d, i), jnp.where(late, g, qd), jnp.where(late, h, qi),
                jnp.where(again, e, od), jnp.where(again, f, oi), gone + on.astype(jnp.int32))

    zero, one_ = jnp.int32(0), jnp.int32(1)
    state = lax.fori_loop(0, SLOTS, step, (
        one_, start(p, one_), one_, start(q, one_), zero, start(p, zero), first_slots))
    qd, qi, od, oi = state[2:6]
    left = zero
    for more in range(2):
        _, _, _, on_low, on_high = bounds(p, od + more)
        left = jnp.where((oi >= 0) & (on_low < on_high), first_slots + 2, left)
    lax.fori_loop(0, left, lambda m, cur: left_onward(SLOTS - 2 + m, *cur), (od, oi))

    def drain(m, cur):
        qd, qi = cur
        s, there, _ = look(q, qd, qi)

        @pl.when(there)
        def _():
            land(s, qi, osem.at[m % LAPS])
            use(s, qi)

        return advance(q, qd, qi)

    lax.fori_loop(SLOTS - later, SLOTS, drain, (qd, qi))


def round_kernel(x_ref, o_ref, buf, sem):
    chunks, step = 16, 64
    rows = x_ref.shape[0] // chunks
    step = min(step, rows)

    def one(j, carry):
        def some(m, carry):
            part = pl.ds(pl.multiple_of(j * rows + m * step, step), step)
            buf[part, :] = x_ref[part, :].astype(buf.dtype)
            return carry

        lax.fori_loop(0, rows // step, some, 0)
        part = pl.ds(pl.multiple_of(j * rows, rows), rows)
        pltpu.make_async_copy(buf.at[part, :], o_ref.at[part, :], sem).start()
        return carry

    lax.fori_loop(0, chunks, one, 0)
    pltpu.make_async_copy(buf, o_ref, sem).wait()


def solution(mesh):
    chips = mesh.shape["col"] // 2

    def local(l_cols, b_cols):
        order, width = b_cols.shape
        nb = order // BLOCK
        strips = sum(nb - 1 - 2 * s for s in range(nb // 2))
        l_cols = pltpu.with_memory_space_constraint(l_cols, pltpu.HBM)
        b_cols = pltpu.with_memory_space_constraint(b_cols, pltpu.HBM)
        acc = pl.pallas_call(
            functools.partial(kernel, nb, chips),
            out_shape=pltpu.VMEM((order, width), jnp.float32),
            in_specs=[pl.BlockSpec(memory_space=pltpu.HBM)] * 2,
            out_specs=pl.BlockSpec(memory_space=pltpu.VMEM),
            scratch_shapes=[
                pltpu.VMEM((strips, 2, BLOCK, BLOCK), jnp.bfloat16),
                pltpu.VMEM((nb, BLOCK + SPARE, BLOCK // 2), jnp.bfloat16),
                pltpu.VMEM((2, BLOCK // 2, BLOCK // 2), jnp.bfloat16),
                pltpu.VMEM((order, width), jnp.bfloat16),
                pltpu.SemaphoreType.DMA((SLOTS,)),
                pltpu.SemaphoreType.DMA((max(nb, LAPS),)),
                pltpu.SemaphoreType.DMA((RING,)),
                pltpu.SemaphoreType.DMA((nb,)),
                pltpu.SemaphoreType.DMA,
                pltpu.SemaphoreType.REGULAR,
            ],
            compiler_params=pltpu.CompilerParams(
                collective_id=0, has_side_effects=True, vmem_limit_bytes=34 * 2**20),
        )(l_cols, b_cols)
        return pl.pallas_call(
            round_kernel,
            out_shape=jax.ShapeDtypeStruct((order, width), jnp.bfloat16),
            in_specs=[pl.BlockSpec(memory_space=pltpu.VMEM)],
            out_specs=pl.BlockSpec(memory_space=pltpu.HBM),
            scratch_shapes=[
                pltpu.VMEM((order, width), jnp.bfloat16),
                pltpu.SemaphoreType.DMA,
            ],
            compiler_params=pltpu.CompilerParams(vmem_limit_bytes=16 * 2**20),
        )(acc)

    return jax.shard_map(local, mesh=mesh, in_specs=(P("batch", "col"), P("batch", "col")),
                         out_specs=P("batch", "col"), check_vma=False)
```
